32 devices in a mesh: shard: 4 (over z), width: 2 (over core), shift: 4 (over y, x).
Axes of the slice: x: 2, y: 2, z: 4, core: 2. Of those that a mesh axis runs over, the one named last changes fastest.
Arguments:
- w_query: bfloat16 [8192, 2048], P(('shift', 'shard'), 'width'), parts along dimension 0, may hold values from -0.125 to 0.125
- low_query: bfloat16 [8192, 16], P(('shift', 'shard')), parts along dimension 0, may hold values from -0.125 to 0.125
- high_query: bfloat16 [64, 2048], P('shift', 'width'), parts along dimension 0, may hold values from -1.5 to 1.5
- w_key: bfloat16 [8192, 512], P(('shift', 'shard'), 'width'), parts along dimension 0, may hold values from -0.125 to 0.125
- low_key: bfloat16 [8192, 16], P(('shift', 'shard')), parts along dimension 0, may hold values from -0.125 to 0.125
- high_key: bfloat16 [64, 512], P('shift', 'width'), parts along dimension 0, may hold values from -1.5 to 1.5
- w_value: bfloat16 [8192, 512], P(('shift', 'shard'), 'width'), parts along dimension 0, may hold values from -0.125 to 0.125
- low_value: bfloat16 [8192, 16], P(('shift', 'shard')), parts along dimension 0, may hold values from -0.125 to 0.125
- high_value: bfloat16 [64, 512], P('shift', 'width'), parts along dimension 0, may hold values from -1.5 to 1.5
- w_mixed: bfloat16 [8192, 2048], P(('shift', 'width'), 'shard'), parts along dimension 0, may hold values from -0.125 to 0.125
- low_mixed: bfloat16 [8192, 16], P(('shift', 'width')), parts along dimension 0, may hold values from -0.125 to 0.125
- high_mixed: bfloat16 [64, 2048], P('shift', 'shard'), parts along dimension 0, may hold values from -1.5 to 1.5
- norm_train: float32 [8192], P(('shift', 'shard', 'width')), parts along dimension 0, may hold values from 0.25 to 1.75
- norm_step: float32 [8192], P(('shift', 'shard', 'width')), parts along dimension 0, may hold values from -0.3 to 0.3
Outputs:
- final_query: bfloat16 [8192, 2048], P(('shift', 'width')), parts along dimension 0
- final_key: bfloat16 [2048, 2048], P(('shift', 'width')), parts along dimension 0
- final_value: bfloat16 [2048, 2048], P(('shift', 'width')), parts along dimension 0
- final_mixed: bfloat16 [8192, 2048], P('shift', 'width'), parts along dimension 0
- serve_norm: bfloat16 [8192], P('shift'), parts along dimension 0
The draws below stay inside these ranges and needn't reach their ends.
There are 4 independent parts, one for each index of `shift`. The reference program is written for one: setup_inputs(seed, part) draws one part's arguments, and reference() takes and returns one part's arrays. A program takes and returns all parts, laid end to end along the dimension named above; each array names one. Nothing has to cross between parts.
All inputs are finite; a program needn't handle non-finite values.
Results may differ from the reference program's by a relative error of at most 0.001.
Values may be sent and summed in bfloat16 or wider, within the bound.
No kernel may reach another device: no remote copies, remote signals or barrier semaphores. Data moves between devices by JAX's collectives and lax.ppermute only.
A program may use at most 64 MiB of HBM per device.

```python
import jax
import jax.numpy as jnp

D_MODEL = 2048
Q_DIM = 2048
KV_DIM = 512
RANK = 16


def levels(key, shape, pieces, low, top_value):
    gain, own = 1.0, jax.random.fold_in(key, 6)
    for dim, shards_of in pieces:
        heights = jnp.exp(jax.random.uniform(jax.random.fold_in(own, dim), (shards_of,), jnp.float32, low / len(pieces), top_value / len(pieces)))
        gain = gain * jnp.repeat(heights, shape[dim] // shards_of).reshape([-1 if axis == dim else 1 for axis in range(len(shape))])
    return gain


def noise(own_key, shape, width, bound, shards=(), dtype=jnp.bfloat16):
    array = width * jax.random.normal(own_key, shape, jnp.float32)
    if shards:
        array = array * levels(own_key, shape, shards, -0.22, 0.18)
    return jnp.clip(array, -bound, bound).astype(dtype)


def setup_inputs(seed: int = 0, part: int = 0) -> dict:
    keys = jax.random.split(jax.random.key(seed), 15)
    own_keys = jax.random.split(jax.random.fold_in(keys[14], part), 15)
    w_query = noise(own_keys[0], (D_MODEL, Q_DIM), D_MODEL ** -0.5, 0.125, ((0, 4), (1, 2)))
    low_query = noise(own_keys[1], (D_MODEL, RANK), D_MODEL ** -0.5, 0.125, ((0, 4),))
    high_query = noise(own_keys[2], (RANK, Q_DIM), RANK ** -0.5, 1.5, ((1, 2),))
    w_key = noise(own_keys[3], (D_MODEL, KV_DIM), D_MODEL ** -0.5, 0.125, ((0, 4), (1, 2)))
    low_key = noise(own_keys[4], (D_MODEL, RANK), D_MODEL ** -0.5, 0.125, ((0, 4),))
    high_key = noise(own_keys[5], (RANK, KV_DIM), RANK ** -0.5, 1.5, ((1, 2),))
    w_value = noise(own_keys[6], (D_MODEL, KV_DIM), D_MODEL ** -0.5, 0.125, ((0, 4), (1, 2)))
    low_value = noise(own_keys[7], (D_MODEL, RANK), D_MODEL ** -0.5, 0.125, ((0, 4),))
    high_value = noise(own_keys[8], (RANK, KV_DIM), RANK ** -0.5, 1.5, ((1, 2),))
    w_mixed = noise(own_keys[9], (Q_DIM, D_MODEL), Q_DIM ** -0.5, 0.125, ((0, 2), (1, 4)))
    low_mixed = noise(own_keys[10], (Q_DIM, RANK), Q_DIM ** -0.5, 0.125, ((0, 2),))
    high_mixed = noise(own_keys[11], (RANK, D_MODEL), RANK ** -0.5, 1.5, ((1, 4),))
    norm_train = jnp.clip(1.0 + 0.15 * jax.random.normal(own_keys[12], (D_MODEL,), jnp.float32), 0.25, 1.75)
    norm_step = jnp.clip(jax.random.uniform(own_keys[13], (D_MODEL,), jnp.float32, -0.3, 0.3) * levels(own_keys[13], (D_MODEL,), ((0, 8),), -0.4, 0.0), -0.3, 0.3)
    return dict(w_query=w_query, low_query=low_query, high_query=high_query, w_key=w_key, low_key=low_key, high_key=high_key, w_value=w_value, low_value=low_value, high_value=high_value, w_mixed=w_mixed, low_mixed=low_mixed, high_mixed=high_mixed, norm_train=norm_train, norm_step=norm_step)


mix_rate = 0.5


def reference(w_query, low_query, high_query, w_key, low_key, high_key, w_value, low_value, high_value, w_mixed, low_mixed, high_mixed, norm_train, norm_step):
    result_query = w_query.astype(jnp.float32) + mix_rate * jnp.dot(low_query, high_query, preferred_element_type=jnp.float32)
    result_key = w_key.astype(jnp.float32) + mix_rate * jnp.dot(low_key, high_key, preferred_element_type=jnp.float32)
    result_value = w_value.astype(jnp.float32) + mix_rate * jnp.dot(low_value, high_value, preferred_element_type=jnp.float32)
    result_mixed = w_mixed.astype(jnp.float32) + mix_rate * jnp.dot(low_mixed, high_mixed, preferred_element_type=jnp.float32)
    final_query = result_query.T.astype(jnp.bfloat16)
    final_key = result_key.T.astype(jnp.bfloat16)
    final_value = result_value.T.astype(jnp.bfloat16)
    final_mixed = result_mixed.T.astype(jnp.bfloat16)
    serve_norm = (norm_train + norm_step).astype(jnp.bfloat16)
    return final_query, final_key, final_value, final_mixed, serve_norm
```

```python
import functools

import jax
import jax.numpy as jnp
from jax import lax
from jax.experimental import pallas as pl
from jax.experimental.pallas import tpu as pltpu
from jax.sharding import PartitionSpec as P

mix_rate = 0.5
lanes = 128


def merged_transpose_body(w_ref, low_ref, high_ref, out_ref):
    delta = lax.dot_general(
        high_ref[...],
        low_ref[...],
        (((0,), (0,)), ((), ())),
        preferred_element_type=jnp.float32,
    )
    base = w_ref[...].T.astype(jnp.float32)
    out_ref[...] = (base + mix_rate * delta).astype(jnp.bfloat16)


def merged_transpose(w, low, high, block):
    rows, columns = w.shape
    rank = low.shape[1]
    block = min(block, columns)
    return pl.pallas_call(
        merged_transpose_body,
        grid=(columns // block,),
        in_specs=[
            pl.BlockSpec((rows, block), lambda i: (0, i)),
            pl.BlockSpec((rank, rows), lambda i: (0, 0)),
            pl.BlockSpec((rank, block), lambda i: (0, i)),
        ],
        out_specs=pl.BlockSpec((block, rows), lambda i: (i, 0)),
        out_shape=jax.ShapeDtypeStruct((columns, rows), jnp.bfloat16),
        compiler_params=pltpu.CompilerParams(vmem_limit_bytes=12 << 20),
    )(w, low.T, high)


def place_body(count, axis, offsets, *refs):
    pieces, out_ref, sems = refs[: len(offsets)], refs[-2], refs[-1]
    me = lax.axis_index("shard")
    for act in ("start", "wait"):
        for j, (piece, offset) in enumerate(zip(pieces, offsets)):
            extent = piece.shape[axis]
            owner = me + offset

            @pl.when(jnp.logical_and(owner >= 0, owner < count))
            def _():
                start = pl.multiple_of(owner * extent, lanes)
                where = [slice(None), slice(None)]
                where[axis] = pl.ds(start, extent)
                copy = pltpu.make_async_copy(piece, out_ref.at[tuple(where)], sems.at[j])
                getattr(copy, act)()


def place(out, pieces, count, axis):
    arrays = [array for array, _ in pieces]
    offsets = [offset for _, offset in pieces]
    shape = list(arrays[0].shape)
    shape[axis] *= count
    operands = arrays + ([] if out is None else [out])
    anywhere = pl.BlockSpec(memory_space=pl.ANY)
    return pl.pallas_call(
        functools.partial(place_body, count, axis, offsets),
        in_specs=[anywhere] * len(operands),
        out_specs=anywhere,
        out_shape=jax.ShapeDtypeStruct(tuple(shape), jnp.bfloat16),
        scratch_shapes=[pltpu.SemaphoreType.DMA((len(arrays),))],
        input_output_aliases={} if out is None else {len(arrays): 0},
        compiler_params=pltpu.CompilerParams(vmem_limit_bytes=1 << 20),
    )(*operands)


def gathered_norm(norm_train, norm_step):
    return lax.all_gather(
        (norm_train + norm_step).astype(jnp.bfloat16), ("shard", "width"), axis=0, tiled=True
    )


def by_line(count, weights, norm_train, norm_step):
    axes = (1, 1, 1, 0)
    order = (1, 0, 3, 2)
    own = {}
    for j in order:
        w, low, high = weights[j]
        own[j] = merged_transpose(w, low, high, 256)
    up, down = dict(own), dict(own)
    pieces = {j: [(own[j], 0)] for j in order}
    outs = {}
    for step in range(1, count):
        send_up = [(i, i + 1) for i in range(step - 1, count - 1)]
        send_down = [(i + 1, i) for i in range(count - step)]
        for j in order:
            up[j] = lax.ppermute(up[j], "shard", send_up)
            down[j] = lax.ppermute(down[j], "shard", send_down)
            if step == count - 1:
                outs[j] = place(None, pieces[j], count, axes[j])
                pieces[j] = []
            pieces[j] += [(up[j], -step), (down[j], step)]
    for j in order:
        outs[j] = place(outs[j], pieces[j], count, axes[j])
    return (*(outs[j] for j in range(4)), gathered_norm(norm_train, norm_step))


def by_gather(weights, norm_train, norm_step):
    finals = []
    for j, (w, low, high) in enumerate(weights):
        result = w.astype(jnp.float32) + mix_rate * jnp.dot(
            low, high, preferred_element_type=jnp.float32
        )
        narrow = result.astype(jnp.bfloat16)
        finals.append(lax.all_gather(narrow, "shard", axis=1 if j == 3 else 0, tiled=True).T)
    return (*finals, gathered_norm(norm_train, norm_step))


def on_device(count, *args):
    weights, norms = [args[3 * j : 3 * j + 3] for j in range(4)], args[12:]
    aligned = all(size % lanes == 0 for w, _, _ in weights for size in w.shape)
    if count > 2 and aligned:
        return by_line(count, weights, *norms)
    return by_gather(weights, *norms)


def solution(mesh):
    column_cut = (P(("shift", "shard"), "width"), P(("shift", "shard"), None), P("shift", "width"))
    row_cut = (P(("shift", "width"), "shard"), P(("shift", "width"), None), P("shift", "shard"))
    norm = P(("shift", "shard", "width"))
    return jax.shard_map(
        functools.partial(on_device, mesh.shape["shard"]),
        mesh=mesh,
        in_specs=(*column_cut, *column_cut, *column_cut, *row_cut, norm, norm),
        out_specs=(
            P(("shift", "width"), None),
            P(("shift", "width"), None),
            P(("shift", "width"), None),
            P("shift", "width"),
            P("shift"),
        ),
        check_vma=False,
    )
```

```python
import functools

import jax
import jax.numpy as jnp
from jax import lax
from jax.experimental import pallas as pl
from jax.experimental.pallas import tpu as pltpu
from jax.sharding import PartitionSpec as P

mix_rate = 0.5
lanes = 128
sublanes = 8


in_vmem = pl.BlockSpec(memory_space=pltpu.VMEM)
in_hbm = pl.BlockSpec(memory_space=pltpu.HBM)


def merge_body(count, block, extra, *refs):
    sources = refs[: 3 * count]
    row_ref = refs[3 * count] if extra else None
    out_ref = refs[3 * count + extra]
    held = refs[3 * count + extra + 1 : -1]
    sems = refs[-1]
    copies = []
    for j in range(count):
        w, low, high = sources[3 * j : 3 * j + 3]
        w_held, low_held, high_held = held[3 * j : 3 * j + 3]
        columns = w.shape[1]
        pairs = [(low, low_held), (high, high_held)]
        for first in range(0, columns, block):
            part = (slice(None), pl.ds(first, block))
            pairs.append((w.at[part], w_held.at[part]))
        for source, target in pairs:
            copies.append(pltpu.make_async_copy(source, target, sems.at[len(copies)]))
    for copy in copies:
        copy.start()
    waits = iter(copies)
    base = 0
    for j in range(count):
        w_held, low_held, high_held = held[3 * j : 3 * j + 3]
        columns = w_held.shape[1]
        next(waits).wait()
        next(waits).wait()
        for first in range(0, columns, block):
            next(waits).wait()
            part = pl.ds(first, block)
            delta = lax.dot_general(
                high_held[:, part],
                low_held[...],
                (((0,), (0,)), ((), ())),
                preferred_element_type=jnp.float32,
            )
            kept = w_held[:, part].T.astype(jnp.float32)
            out_ref[pl.ds(base + first, block), :] = (kept + mix_rate * delta).astype(jnp.bfloat16)
        base += columns
    if extra:
        out_ref[pl.ds(base, sublanes), :] = jnp.broadcast_to(
            row_ref[...], (sublanes, row_ref.shape[1])
        )


def merged(weights, block, row=None):
    rows = weights[0][0].shape[0]
    columns = sum(w.shape[1] for w, _, _ in weights)
    extra = int(row is not None)
    operands, held, parts = [], [], 0
    for w, low, high in weights:
        operands += [w, low.T, high]
        held += [pltpu.VMEM(array.shape, array.dtype) for array in operands[-3:]]
        parts += 2 + w.shape[1] // block
    operands = [pltpu.with_memory_space_constraint(array, pltpu.HBM) for array in operands]
    return pl.pallas_call(
        functools.partial(merge_body, len(weights), block, extra),
        in_specs=[in_hbm] * len(operands) + [in_vmem] * extra,
        out_specs=in_vmem,
        out_shape=jax.ShapeDtypeStruct((columns + sublanes * extra, rows), jnp.bfloat16),
        scratch_shapes=[*held, pltpu.SemaphoreType.DMA((parts,))],
        compiler_params=pltpu.CompilerParams(vmem_limit_bytes=12 << 20),
    )(*operands, *([row] if extra else []))


def place_body(count, targets, offsets, *refs):
    pieces, outs, sems = refs[: len(offsets)], refs[-1 - len(targets) : -1], refs[-1]
    me = lax.axis_index("shard")
    for act in ("start", "wait"):
        for j, (piece, offset) in enumerate(zip(pieces, offsets)):
            owner = me + offset

            @pl.when(jnp.logical_and(owner >= 0, owner < count))
            def _():
                base = 0
                for t, (rows, axis) in enumerate(targets):
                    extent = rows if axis == 0 else piece.shape[1]
                    start = pl.multiple_of(owner * extent, sublanes if axis == 0 else lanes)
                    where = [slice(None), slice(None)]
                    where[axis] = pl.ds(start, extent)
                    copy = pltpu.make_async_copy(
                        piece.at[pl.ds(base, rows)], outs[t].at[tuple(where)], sems.at[j, t]
                    )
                    getattr(copy, act)()
                    base += rows


def place(outs, pieces, count, targets):
    arrays = [array for array, _ in pieces]
    offsets = [offset for _, offset in pieces]
    width = arrays[0].shape[1]
    shapes = [
        jax.ShapeDtypeStruct((rows * count, width) if axis == 0 else (rows, width * count), jnp.bfloat16)
        for rows, axis in targets
    ]
    return pl.pallas_call(
        functools.partial(place_body, count, targets, offsets),
        in_specs=[in_vmem] * len(arrays) + [in_hbm] * len(outs),
        out_specs=[in_hbm] * len(targets),
        out_shape=shapes,
        scratch_shapes=[pltpu.SemaphoreType.DMA((len(arrays), len(targets)))],
        input_output_aliases={len(arrays) + t: t for t in range(len(outs))},
        compiler_params=pltpu.CompilerParams(vmem_limit_bytes=1 << 20),
    )(*arrays, *outs)


def by_line(count, query, key, value, mixed, norms):
    first = merged([mixed], 256)
    first, norms, query = lax.optimization_barrier((first, norms, query))
    row = lax.all_gather((norms[0] + norms[1]).astype(jnp.bfloat16), "width", axis=0, tiled=True)
    second = merged([query], 256, row[None])
    second, key, value = lax.optimization_barrier((second, key, value))
    own = [first, second, merged([key, value], 256)]
    targets = [
        ((mixed[0].shape[1], 0),),
        ((query[0].shape[1], 1), (sublanes, 0)),
        ((key[0].shape[1], 1), (value[0].shape[1], 1)),
    ]
    chunks = range(len(own))
    up, down = list(own), list(own)
    ready = [[(piece, 0)] for piece in own]
    outs = [[] for _ in own]
    for step in range(1, count):
        send_up = [(i, i + 1) for i in range(step - 1, count - 1)]
        send_down = [(i + 1, i) for i in range(count - step)]
        for c in chunks:
            if step > 2:
                tied = outs if c == chunks[-1] else [outs[c]]
                up[c], down[c], tied = lax.optimization_barrier((up[c], down[c], tied))
                if c == chunks[-1]:
                    outs = tied
                else:
                    outs[c] = tied[0]
            up[c] = lax.ppermute(up[c], "shard", send_up)
            down[c] = lax.ppermute(down[c], "shard", send_down)
            if step > 1:
                outs[c] = place(outs[c], ready[c], count, targets[c])
                ready[c] = []
            ready[c] += [(up[c], -step), (down[c], step)]
    for c in chunks:
        outs[c] = place(outs[c], ready[c], count, targets[c])
    final_mixed, final_query, norms = outs[0][0], outs[1][0], outs[1][1]
    serve_norm = norms.reshape(count, sublanes, -1)[:, 0].reshape(-1)
    return final_query, *outs[2], final_mixed, serve_norm


def by_gather(count, query, key, value, mixed, norms):
    finals = []
    for axis, (w, low, high) in ((0, query), (0, key), (0, value), (1, mixed)):
        result = w.astype(jnp.float32) + mix_rate * jnp.dot(
            low, high, preferred_element_type=jnp.float32
        )
        narrow = result.astype(jnp.bfloat16)
        finals.append(lax.all_gather(narrow, "shard", axis=axis, tiled=True).T)
    norm = (norms[0] + norms[1]).astype(jnp.bfloat16)
    serve_norm = lax.all_gather(norm, ("shard", "width"), axis=0, tiled=True)
    return *finals, serve_norm


def on_device(count, *args):
    weights = [args[3 * j : 3 * j + 3] for j in range(4)]
    aligned = all(size % (2 * lanes) == 0 for w, _, _ in weights for size in w.shape)
    form = by_line if count > 2 and aligned else by_gather
    return form(count, *weights, args[12:])


def solution(mesh):
    column_cut = (P(("shift", "shard"), "width"), P(("shift", "shard"), None), P("shift", "width"))
    row_cut = (P(("shift", "width"), "shard"), P(("shift", "width"), None), P("shift", "shard"))
    norm = P(("shift", "shard", "width"))
    return jax.shard_map(
        functools.partial(on_device, mesh.shape["shard"]),
        mesh=mesh,
        in_specs=(*column_cut, *column_cut, *column_cut, *row_cut, norm, norm),
        out_specs=(
            P(("shift", "width"), None),
            P(("shift", "width"), None),
            P(("shift", "width"), None),
            P("shift", "width"),
            P("shift"),
        ),
        check_vma=False,
    )
```

```python
import functools

import jax
import jax.numpy as jnp
from jax import lax
from jax.experimental import pallas as pl
from jax.experimental.pallas import tpu as pltpu
from jax.sharding import PartitionSpec as P


mix_rate = 0.5
lanes = 128
sublanes = 8


in_vmem = pl.BlockSpec(memory_space=pltpu.VMEM)
in_hbm = pl.BlockSpec(memory_space=pltpu.HBM)


def merge_body(count, block, extra, *refs):
    sources = refs[: 3 * count]
    row_ref = refs[3 * count] if extra else None
    out_ref = refs[3 * count + extra]
    held = refs[3 * count + extra + 1 : -1]
    sems = refs[-1]
    copies = []
    for j in range(count):
        w, low, high = sources[3 * j : 3 * j + 3]
        w_held, low_held, high_held = held[3 * j : 3 * j + 3]
        columns = w.shape[1]
        pairs = [(low, low_held), (high, high_held)]
        for first in range(0, columns, block):
            part = (slice(None), pl.ds(first, block))
            pairs.append((w.at[part], w_held.at[part]))
        for source, target in pairs:
            copies.append(pltpu.make_async_copy(source, target, sems.at[len(copies)]))
    for copy in copies:
        copy.start()
    waits = iter(copies)
    base = 0
    for j in range(count):
        w_held, low_held, high_held = held[3 * j : 3 * j + 3]
        columns = w_held.shape[1]
        next(waits).wait()
        next(waits).wait()
        for first in range(0, columns, block):
            next(waits).wait()
            part = pl.ds(first, block)
            delta = lax.dot_general(
                high_held[:, part],
                low_held[...],
                (((0,), (0,)), ((), ())),
                preferred_element_type=jnp.float32,
            )
            kept = w_held[:, part].T.astype(jnp.float32)
            out_ref[pl.ds(base + first, block), :] = (kept + mix_rate * delta).astype(jnp.bfloat16)
        base += columns
    if extra:
        out_ref[pl.ds(base, sublanes), :] = jnp.broadcast_to(
            row_ref[...], (sublanes, row_ref.shape[1])
        )


def merged(weights, block, row=None):
    rows = weights[0][0].shape[0]
    columns = sum(w.shape[1] for w, _, _ in weights)
    extra = int(row is not None)
    operands, held, parts = [], [], 0
    for w, low, high in weights:
        operands += [w, low.T, high]
        held += [pltpu.VMEM(array.shape, array.dtype) for array in operands[-3:]]
        parts += 2 + w.shape[1] // block
    operands = [pltpu.with_memory_space_constraint(array, pltpu.HBM) for array in operands]
    return pl.pallas_call(
        functools.partial(merge_body, len(weights), block, extra),
        in_specs=[in_hbm] * len(operands) + [in_vmem] * extra,
        out_specs=in_vmem,
        out_shape=jax.ShapeDtypeStruct((columns + sublanes * extra, rows), jnp.bfloat16),
        scratch_shapes=[*held, pltpu.SemaphoreType.DMA((parts,))],
        compiler_params=pltpu.CompilerParams(vmem_limit_bytes=12 << 20),
    )(*operands, *([row] if extra else []))


def place_body(count, targets, offsets, *refs):
    pieces, outs, sems = refs[: len(offsets)], refs[-1 - len(targets) : -1], refs[-1]
    me = lax.axis_index("shard")
    sign = 1 - 2 * lax.rem(me, 2)
    for act in ("start", "wait"):
        for j, (piece, offset) in enumerate(zip(pieces, offsets)):
            owner = me + sign * offset

            @pl.when(jnp.logical_and(owner >= 0, owner < count))
            def _():
                base = 0
                for t, (rows, axis) in enumerate(targets):
                    extent = rows if axis == 0 else piece.shape[1]
                    start = pl.multiple_of(owner * extent, sublanes if axis == 0 else lanes)
                    where = [slice(None), slice(None)]
                    where[axis] = pl.ds(start, extent)
                    copy = pltpu.make_async_copy(
                        piece.at[pl.ds(base, rows)], outs[t].at[tuple(where)], sems.at[j, t]
                    )
                    getattr(copy, act)()
                    base += rows


def place(outs, pieces, count, targets):
    arrays = [array for array, _ in pieces]
    offsets = [offset for _, offset in pieces]
    width = arrays[0].shape[1]
    shapes = [
        jax.ShapeDtypeStruct((rows * count, width) if axis == 0 else (rows, width * count), jnp.bfloat16)
        for rows, axis in targets
    ]
    return pl.pallas_call(
        functools.partial(place_body, count, targets, offsets),
        in_specs=[in_vmem] * len(arrays) + [in_hbm] * len(outs),
        out_specs=[in_hbm] * len(targets),
        out_shape=shapes,
        scratch_shapes=[pltpu.SemaphoreType.DMA((len(arrays), len(targets)))],
        input_output_aliases={len(arrays) + t: t for t in range(len(outs))},
        compiler_params=pltpu.CompilerParams(vmem_limit_bytes=1 << 20),
    )(*arrays, *outs)


def hops(count):
    plan = []
    for k in range(1, count):
        for name, source, parity in (("a", "b", 0), ("b", "a", 1)):
            pairs = []
            for i in range(parity, count - 1, 2):
                if i + k < count:
                    pairs.append((i + 1, i))
                if i + 1 - k >= 0:
                    pairs.append((i, i + 1))
            if pairs:
                offset = k if parity == 0 else -k
                plan.append((f"{name}{k}", f"{source}{k - 1}", pairs, offset))
    return plan


def by_line(count, query, key, value, mixed, norms):
    first = merged([mixed], 256)
    pair = lax.all_gather((norms[0] + norms[1]).astype(jnp.bfloat16), "width", axis=0, tiled=True)
    second = merged([query], 256, pair[None])
    third = merged([key, value], 256)
    own = [first, second, third]
    targets = [
        ((mixed[0].shape[1], 0),),
        ((query[0].shape[1], 1), (sublanes, 0)),
        ((key[0].shape[1], 1), (value[0].shape[1], 1)),
    ]
    plan = hops(count)
    outs = []
    for c, piece in enumerate(own):
        held = {"a0": piece, "b0": piece}
        arrived = [(piece, 0)]
        out = []
        for k in range(1, count):
            for name, source, pairs, offset in plan:
                if int(name[1:]) == k:
                    held[name] = lax.ppermute(held[source], "shard", pairs)
                    arrived.append((held[name], offset))
            out = place(out, arrived, count, targets[c])
            arrived = []
        outs.append(out)
    final_mixed, final_query, rows = outs[0][0], outs[1][0], outs[1][1]
    serve_norm = rows.reshape(count, sublanes, -1)[:, 0].reshape(-1)
    return final_query, *outs[2], final_mixed, serve_norm


def by_gather(count, query, key, value, mixed, norms):
    finals = []
    for axis, (w, low, high) in ((0, query), (0, key), (0, value), (1, mixed)):
        result = w.astype(jnp.float32) + mix_rate * jnp.dot(
            low, high, preferred_element_type=jnp.float32
        )
        narrow = result.astype(jnp.bfloat16)
        finals.append(lax.all_gather(narrow, "shard", axis=axis, tiled=True).T)
    norm = (norms[0] + norms[1]).astype(jnp.bfloat16)
    serve_norm = lax.all_gather(norm, ("shard", "width"), axis=0, tiled=True)
    return *finals, serve_norm


def on_device(form, count, *args):
    weights = [args[3 * j : 3 * j + 3] for j in range(4)]
    return form(count, *weights, args[12:])


def solution(mesh):
    column_cut = (P(("shift", "shard"), "width"), P(("shift", "shard"), None), P("shift", "width"))
    row_cut = (P(("shift", "width"), "shard"), P(("shift", "width"), None), P("shift", "shard"))
    norm = P(("shift", "shard", "width"))
    count = mesh.shape["shard"]

    def step(*args):
        rows = args[0].shape[0] // (mesh.shape["shift"] * count)
        columns = args[9].shape[1] // count
        narrow = [args[j].shape[1] // mesh.shape["width"] for j in (0, 3, 6)]
        aligned = all(size % (2 * lanes) == 0 for size in (rows, columns, *narrow))
        line = count > 2 and aligned
        program = jax.shard_map(
            functools.partial(on_device, by_line if line else by_gather, count),
            mesh=mesh,
            in_specs=(*column_cut, *column_cut, *column_cut, *row_cut, norm, norm),
            out_specs=(
                P(("shift", "width"), None),
                P(("shift", "width"), None),
                P(("shift", "width"), None),
                P("shift", "width"),
                P("shift"),
            ),
            check_vma=False,
        )
        return program(*args)

    return step
```

```python
import functools

import jax
import jax.numpy as jnp
from jax import lax
from jax.experimental import pallas as pl
from jax.experimental.pallas import tpu as pltpu
from jax.sharding import PartitionSpec as P


mix_rate = 0.5
lanes = 128
sublanes = 8


in_vmem = pl.BlockSpec(memory_space=pltpu.VMEM)
in_hbm = pl.BlockSpec(memory_space=pltpu.HBM)


def merge_body(first, blocks, w_ref, low_ref, high_ref, out_ref, w_held, low_held, high_held, sems):
    total = sum(blocks)
    copies = [
        pltpu.make_async_copy(low_ref, low_held, sems.at[0]),
        pltpu.make_async_copy(high_ref.at[:, pl.ds(first, total)], high_held, sems.at[1]),
    ]
    base = 0
    for j, block in enumerate(blocks):
        copies.append(
            pltpu.make_async_copy(
                w_ref.at[:, pl.ds(first + base, block)], w_held.at[:, pl.ds(base, block)], sems.at[2 + j]
            )
        )
        base += block
    for copy in copies:
        copy.start()
    copies[0].wait()
    copies[1].wait()
    base = 0
    for j, block in enumerate(blocks):
        copies[2 + j].wait()
        part = pl.ds(base, block)
        delta = lax.dot_general(
            high_held[:, part],
            low_held[...],
            (((0,), (0,)), ((), ())),
            preferred_element_type=jnp.float32,
        )
        kept = w_held[:, part].T.astype(jnp.float32)
        out_ref[part, :] = (kept + mix_rate * delta).astype(jnp.bfloat16)
        base += block


def merged(w, low, high, first, last):
    rows, total, rank = w.shape[0], last - first, low.shape[1]
    block = 2 * lanes
    blocks = [min(block, total - base) for base in range(0, total, block)]
    operands = [pltpu.with_memory_space_constraint(a, pltpu.HBM) for a in (w, low.T, high)]
    return pl.pallas_call(
        functools.partial(merge_body, first, blocks),
        in_specs=[in_hbm] * 3,
        out_specs=in_vmem,
        out_shape=jax.ShapeDtypeStruct((total, rows), jnp.bfloat16),
        scratch_shapes=[
            pltpu.VMEM((rows, total), jnp.bfloat16),
            pltpu.VMEM((rank, rows), jnp.bfloat16),
            pltpu.VMEM((rank, total), jnp.bfloat16),
            pltpu.SemaphoreType.DMA((2 + len(blocks),)),
        ],
        compiler_params=pltpu.CompilerParams(vmem_limit_bytes=12 << 20),
    )(*operands)


def sum_body(train_ref, step_ref, out_ref):
    out_ref[...] = jnp.zeros_like(out_ref)
    out_ref[: train_ref.shape[0], :] = (train_ref[...] + step_ref[...]).astype(jnp.bfloat16)


def summed(train, step):
    used = train.size // lanes
    tall = -(-used // sublanes) * sublanes
    return pl.pallas_call(
        sum_body,
        in_specs=[in_vmem] * 2,
        out_specs=in_vmem,
        out_shape=jax.ShapeDtypeStruct((tall, lanes), jnp.bfloat16),
        compiler_params=pltpu.CompilerParams(vmem_limit_bytes=1 << 20),
    )(train.reshape(used, lanes), step.reshape(used, lanes))


def place_body(count, axis, extent, base, offsets, *refs):
    pieces, out_ref, sems = refs[: len(offsets)], refs[-2], refs[-1]
    me = lax.axis_index("shard")
    sign = 1 - 2 * lax.rem(me, 2)
    for act in ("start", "wait"):
        for j, (piece, offset) in enumerate(zip(pieces, offsets)):
            owner = me + sign * offset

            @pl.when(jnp.logical_and(owner >= 0, owner < count))
            def _():
                start = pl.multiple_of(owner * extent + base, (sublanes, lanes)[axis])
                where = [slice(None), slice(None)]
                where[axis] = pl.ds(start, piece.shape[axis])
                copy = pltpu.make_async_copy(piece, out_ref.at[tuple(where)], sems.at[j])
                getattr(copy, act)()


def place(out, pieces, count, axis, extent, base):
    arrays = [array for array, _ in pieces]
    offsets = [offset for _, offset in pieces]
    shape = list(arrays[0].shape)
    shape[axis] = count * extent
    operands = arrays + ([] if out is None else [out])
    return pl.pallas_call(
        functools.partial(place_body, count, axis, extent, base, offsets),
        in_specs=[in_vmem] * len(arrays) + [in_hbm] * (len(operands) - len(arrays)),
        out_specs=in_hbm,
        out_shape=jax.ShapeDtypeStruct(tuple(shape), jnp.bfloat16),
        scratch_shapes=[pltpu.SemaphoreType.DMA((len(arrays),))],
        input_output_aliases={} if out is None else {len(arrays): 0},
        compiler_params=pltpu.CompilerParams(vmem_limit_bytes=4 << 20),
    )(*operands)


def hops(count):
    plan = []
    for k in range(1, count):
        for name, source, parity in (("a", "b", 0), ("b", "a", 1)):
            pairs = []
            for i in range(parity, count - 1, 2):
                if i + k < count:
                    pairs.append((i + 1, i))
                if i + 1 - k >= 0:
                    pairs.append((i, i + 1))
            if pairs:
                offset = k if parity == 0 else -k
                plan.append((f"{name}{k}", f"{source}{k - 1}", pairs, offset))
    return plan


chunk_names = ("mixed_head", "mixed_rest", "query", "norm", "key", "value")


def by_line(count, query, key, value, mixed, norms):
    columns = mixed[0].shape[1]
    pieces, where = {}, {}

    def chunk(name, weight, axis, extent, first, last):
        pieces[name] = merged(*weight, first, last)
        where[name] = (axis, extent, first if axis == 0 else 0)

    chunk("mixed_head", mixed, 0, columns, 0, lanes)
    chunk("mixed_rest", mixed, 0, columns, lanes, columns)
    for name, weight in (("query", query), ("key", key), ("value", value)):
        chunk(name, weight, 1, weight[0].shape[0], 0, weight[0].shape[1])
    row = summed(*norms)
    pieces["norm"] = lax.all_gather(row, "width", axis=0, tiled=True)
    where["norm"] = (0, pieces["norm"].shape[0], 0)

    plan = hops(count)
    outs = {}
    held = {name: {"a0": piece, "b0": piece} for name, piece in pieces.items()}
    arrived = {name: [(piece, 0)] for name, piece in pieces.items()}
    for k in range(1, count):
        for name in chunk_names:
            for hop, source, pairs, offset in plan:
                if int(hop[1:]) == k:
                    held[name][hop] = lax.ppermute(held[name][source], "shard", pairs)
                    arrived[name].append((held[name][hop], offset))
            target = name.split("_")[0]
            outs[target] = place(outs.get(target), arrived[name], count, *where[name])
            arrived[name] = []
    used = norms[0].size // lanes
    serve_norm = outs["norm"].reshape(-1, row.shape[0], lanes)[:, :used].reshape(-1)
    return outs["query"], outs["key"], outs["value"], outs["mixed"], serve_norm


def by_gather(count, query, key, value, mixed, norms):
    finals = []
    for axis, (w, low, high) in ((0, query), (0, key), (0, value), (1, mixed)):
        result = w.astype(jnp.float32) + mix_rate * jnp.dot(
            low, high, preferred_element_type=jnp.float32
        )
        narrow = result.astype(jnp.bfloat16)
        finals.append(lax.all_gather(narrow, "shard", axis=axis, tiled=True).T)
    norm = (norms[0] + norms[1]).astype(jnp.bfloat16)
    serve_norm = lax.all_gather(norm, ("shard", "width"), axis=0, tiled=True)
    return *finals, serve_norm


def on_device(form, count, *args):
    weights = [args[3 * j : 3 * j + 3] for j in range(4)]
    return form(count, *weights, args[12:])


def solution(mesh):
    column_cut = (P(("shift", "shard"), "width"), P(("shift", "shard"), None), P("shift", "width"))
    row_cut = (P(("shift", "width"), "shard"), P(("shift", "width"), None), P("shift", "shard"))
    norm = P(("shift", "shard", "width"))
    count = mesh.shape["shard"]

    def step(*args):
        rows = args[0].shape[0] // (mesh.shape["shift"] * count)
        columns = args[9].shape[1] // count
        narrow = [args[j].shape[1] // mesh.shape["width"] for j in (0, 3, 6)]
        gains = args[12].shape[0] // (mesh.shape["shift"] * count * mesh.shape["width"])
        aligned = all(size % (2 * lanes) == 0 for size in (rows, columns, *narrow, gains))
        line = count > 2 and aligned
        program = jax.shard_map(
            functools.partial(on_device, by_line if line else by_gather, count),
            mesh=mesh,
            in_specs=(*column_cut, *column_cut, *column_cut, *row_cut, norm, norm),
            out_specs=(
                P(("shift", "width"), None),
                P(("shift", "width"), None),
                P(("shift", "width"), None),
                P("shift", "width"),
                P("shift"),
            ),
            check_vma=False,
        )
        return program(*args)

    return step
```

```python
import functools

import jax
import jax.numpy as jnp
from jax import lax
from jax.experimental import pallas as pl
from jax.experimental.pallas import tpu as pltpu
from jax.sharding import PartitionSpec as P


mix_rate = 0.5
lanes = 128
sublanes = 8


in_vmem = pl.BlockSpec(memory_space=pltpu.VMEM)
in_hbm = pl.BlockSpec(memory_space=pltpu.HBM)


def merge_body(spans, *refs):
    count = len(spans)
    inputs = 3 * sum(span is not None for span in spans) + 2 * sum(span is None for span in spans)
    sources, outs = iter(refs[:inputs]), refs[inputs : inputs + count]
    held, sems = iter(refs[inputs + count : -1]), refs[-1]
    work = []
    used = 0

    def start(source, target):
        nonlocal used
        copy = pltpu.make_async_copy(source, target, sems.at[used])
        copy.start()
        used += 1
        return copy

    for span, out_ref in zip(spans, outs):
        if span is None:
            work.append((next(sources), next(sources), out_ref))
            continue
        first, blocks = span
        w_ref, low_ref, high_ref = (next(sources) for _ in range(3))
        w_held, low_held, high_held = (next(held) for _ in range(3))
        copies = [
            start(low_ref, low_held),
            start(high_ref.at[:, pl.ds(first, sum(blocks))], high_held),
        ]
        base = 0
        parts = []
        for block in blocks:
            part = pl.ds(base, block)
            copies.append(start(w_ref.at[:, pl.ds(first + base, block)], w_held.at[:, part]))
            parts.append(part)
            base += block
        work.append((w_held, low_held, high_held, copies, parts, out_ref))
    for item in work:
        if len(item) == 3:
            train_ref, step_ref, out_ref = item
            out_ref[...] = jnp.zeros_like(out_ref)
            out_ref[: train_ref.shape[0], :] = (train_ref[...] + step_ref[...]).astype(jnp.bfloat16)
            continue
        w_held, low_held, high_held, copies, parts, out_ref = item
        copies[0].wait()
        copies[1].wait()
        for part, copy in zip(parts, copies[2:]):
            copy.wait()
            delta = lax.dot_general(
                high_held[:, part],
                low_held[...],
                (((0,), (0,)), ((), ())),
                preferred_element_type=jnp.float32,
            )
            kept = w_held[:, part].T.astype(jnp.float32)
            out_ref[part, :] = (kept + mix_rate * delta).astype(jnp.bfloat16)


def merged(*tasks):
    spans, operands, specs, shapes, scratch, copies = [], [], [], [], [], 0
    for task in tasks:
        if len(task) == 2:
            used = task[0].size // lanes
            tall = -(-used // sublanes) * sublanes
            spans.append(None)
            operands += [a.reshape(used, lanes) for a in task]
            specs += [in_vmem] * 2
            shapes.append(jax.ShapeDtypeStruct((tall, lanes), jnp.bfloat16))
            continue
        w, low, high, first, last = task
        rows, total, rank = w.shape[0], last - first, low.shape[1]
        block = 2 * lanes
        blocks = [min(block, total - base) for base in range(0, total, block)]
        spans.append((first, blocks))
        operands += [pltpu.with_memory_space_constraint(a, pltpu.HBM) for a in (w, low.T, high)]
        specs += [in_hbm] * 3
        shapes.append(jax.ShapeDtypeStruct((total, rows), jnp.bfloat16))
        scratch += [
            pltpu.VMEM((rows, total), jnp.bfloat16),
            pltpu.VMEM((rank, rows), jnp.bfloat16),
            pltpu.VMEM((rank, total), jnp.bfloat16),
        ]
        copies += 2 + len(blocks)
    return pl.pallas_call(
        functools.partial(merge_body, spans),
        in_specs=specs,
        out_specs=[in_vmem] * len(shapes),
        out_shape=shapes,
        scratch_shapes=[*scratch, pltpu.SemaphoreType.DMA((copies,))],
        compiler_params=pltpu.CompilerParams(vmem_limit_bytes=12 << 20),
    )(*operands)


def place_body(count, moves, outs_at, *refs):
    sems = refs[-1]
    me = lax.axis_index("shard")
    sign = 1 - 2 * lax.rem(me, 2)
    for act in ("start", "wait"):
        for j, (piece, (out, axis, extent, base, offset)) in enumerate(zip(refs, moves)):
            owner = me + sign * offset

            @pl.when(jnp.logical_and(owner >= 0, owner < count))
            def _():
                start = pl.multiple_of(owner * extent + base, (sublanes, lanes)[axis])
                where = [slice(None), slice(None)]
                where[axis] = pl.ds(start, piece.shape[axis])
                copy = pltpu.make_async_copy(piece, refs[outs_at + out].at[tuple(where)], sems.at[j])
                getattr(copy, act)()


def place(outs, pieces, count):
    targets = list(dict.fromkeys(piece[0] for piece in pieces))
    arrays = [piece[-1] for piece in pieces]
    moves = [(targets.index(piece[0]), *piece[1:-1]) for piece in pieces]
    shapes = []
    for target in targets:
        _, axis, extent, _, _, array = next(piece for piece in pieces if piece[0] == target)
        shape = list(array.shape)
        shape[axis] = count * extent
        shapes.append(jax.ShapeDtypeStruct(tuple(shape), jnp.bfloat16))
    kept = [outs[target] for target in targets if target in outs]
    placed = pl.pallas_call(
        functools.partial(place_body, count, moves, len(arrays) + len(kept)),
        in_specs=[in_vmem] * len(arrays) + [in_hbm] * len(kept),
        out_specs=[in_hbm] * len(targets),
        out_shape=shapes,
        scratch_shapes=[pltpu.SemaphoreType.DMA((len(arrays),))],
        input_output_aliases={len(arrays) + j: j for j in range(len(kept))},
        compiler_params=pltpu.CompilerParams(vmem_limit_bytes=4 << 20),
    )(*arrays, *kept)
    outs.update(zip(targets, placed))


def hops(count):
    plan = []
    for k in range(1, count):
        for name, source, parity in (("a", "b", 0), ("b", "a", 1)):
            pairs = []
            for i in range(parity, count - 1, 2):
                if i + k < count:
                    pairs.append((i + 1, i))
                if i + 1 - k >= 0:
                    pairs.append((i, i + 1))
            if pairs:
                offset = k if parity == 0 else -k
                plan.append((f"{name}{k}", f"{source}{k - 1}", pairs, offset))
    return plan


chunk_names = ("mixed_head", "mixed_rest", "query", "norm", "key", "value")


def groups(count):
    whole = (chunk_names,)
    return [whole] * (count - 2) + [(chunk_names[:-2], chunk_names[-2:-1], chunk_names[-1:])]


def by_line(count, query, key, value, mixed, norms):
    rows, columns = query[0].shape[0], mixed[0].shape[1]
    pieces = {}
    (pieces["mixed_head"],) = merged((*mixed, 0, lanes))
    (pieces["mixed_rest"],) = merged((*mixed, lanes, columns))
    pieces["query"], pieces["key"], pieces["value"], row = merged(
        *((*weight, 0, weight[0].shape[1]) for weight in (query, key, value)), norms
    )
    pieces["norm"] = lax.all_gather(row, "width", axis=0, tiled=True)
    where = {
        "mixed_head": ("mixed", 0, columns, 0),
        "mixed_rest": ("mixed", 0, columns, lanes),
        "query": ("query", 1, rows, 0),
        "norm": ("norm", 0, pieces["norm"].shape[0], 0),
        "key": ("key", 1, rows, 0),
        "value": ("value", 1, rows, 0),
    }
    plan = hops(count)
    outs = {}
    held = {name: {"a0": piece, "b0": piece} for name, piece in pieces.items()}
    arrived = {name: [(*where[name], 0, piece)] for name, piece in pieces.items()}
    for k, parts in enumerate(groups(count), start=1):
        for hop, source, pairs, offset in plan:
            if int(hop[1:]) == k:
                for name in chunk_names:
                    held[name][hop] = lax.ppermute(held[name][source], "shard", pairs)
                    arrived[name].append((*where[name], offset, held[name][hop]))
        for part in parts:
            place(outs, [move for name in part for move in arrived[name]], count)
        arrived = {name: [] for name in chunk_names}
    used = norms[0].size // lanes
    serve_norm = outs["norm"].reshape(-1, row.shape[0], lanes)[:, :used].reshape(-1)
    return outs["query"], outs["key"], outs["value"], outs["mixed"], serve_norm


def by_gather(count, query, key, value, mixed, norms):
    finals = []
    for axis, (w, low, high) in ((0, query), (0, key), (0, value), (1, mixed)):
        result = w.astype(jnp.float32) + mix_rate * jnp.dot(
            low, high, preferred_element_type=jnp.float32
        )
        narrow = result.astype(jnp.bfloat16)
        finals.append(lax.all_gather(narrow, "shard", axis=axis, tiled=True).T)
    norm = (norms[0] + norms[1]).astype(jnp.bfloat16)
    serve_norm = lax.all_gather(norm, ("shard", "width"), axis=0, tiled=True)
    return *finals, serve_norm


def on_device(form, count, *args):
    weights = [args[3 * j : 3 * j + 3] for j in range(4)]
    return form(count, *weights, args[12:])


def solution(mesh):
    column_cut = (P(("shift", "shard"), "width"), P(("shift", "shard"), None), P("shift", "width"))
    row_cut = (P(("shift", "width"), "shard"), P(("shift", "width"), None), P("shift", "shard"))
    norm = P(("shift", "shard", "width"))
    count = mesh.shape["shard"]

    def step(*args):
        rows = args[0].shape[0] // (mesh.shape["shift"] * count)
        columns = args[9].shape[1] // count
        narrow = [args[j].shape[1] // mesh.shape["width"] for j in (0, 3, 6)]
        gains = args[12].shape[0] // (mesh.shape["shift"] * count * mesh.shape["width"])
        aligned = all(size % (2 * lanes) == 0 for size in (rows, columns, *narrow, gains))
        line = count > 2 and aligned
        program = jax.shard_map(
            functools.partial(on_device, by_line if line else by_gather, count),
            mesh=mesh,
            in_specs=(*column_cut, *column_cut, *column_cut, *row_cut, norm, norm),
            out_specs=(
                P(("shift", "width"), None),
                P(("shift", "width"), None),
                P(("shift", "width"), None),
                P("shift", "width"),
                P("shift"),
            ),
            check_vma=False,
        )
        return program(*args)

    return step
```

```python
import functools

import jax
import jax.numpy as jnp
from jax import lax
from jax.experimental import pallas as pl
from jax.experimental.pallas import tpu as pltpu
from jax.sharding import PartitionSpec as P


mix_rate = 0.5
lanes = 128
sublanes = 8


in_vmem = pl.BlockSpec(memory_space=pltpu.VMEM)
in_hbm = pl.BlockSpec(memory_space=pltpu.HBM)


def merge_body(spans, *refs):
    count = len(spans)
    inputs = 3 * sum(span is not None for span in spans) + 2 * sum(span is None for span in spans)
    sources, outs = iter(refs[:inputs]), refs[inputs : inputs + count]
    held, sems = iter(refs[inputs + count : -1]), refs[-1]
    work = []
    used = 0

    def start(source, target):
        nonlocal used
        copy = pltpu.make_async_copy(source, target, sems.at[used])
        copy.start()
        used += 1
        return copy

    for span, out_ref in zip(spans, outs):
        if span is None:
            work.append((next(sources), next(sources), out_ref))
            continue
        first, blocks = span
        w_ref, low_ref, high_ref = (next(sources) for _ in range(3))
        w_held, low_held, high_held = (next(held) for _ in range(3))
        copies = [
            start(low_ref, low_held),
            start(high_ref.at[:, pl.ds(first, sum(blocks))], high_held),
        ]
        base = 0
        parts = []
        for block in blocks:
            part = pl.ds(base, block)
            copies.append(start(w_ref.at[:, pl.ds(first + base, block)], w_held.at[:, part]))
            parts.append(part)
            base += block
        work.append((w_held, low_held, high_held, copies, parts, out_ref))
    for item in work:
        if len(item) == 3:
            train_ref, step_ref, out_ref = item
            out_ref[...] = jnp.zeros_like(out_ref)
            out_ref[: train_ref.shape[0], :] = (train_ref[...] + step_ref[...]).astype(jnp.bfloat16)
            continue
        w_held, low_held, high_held, copies, parts, out_ref = item
        copies[0].wait()
        copies[1].wait()
        for part, copy in zip(parts, copies[2:]):
            copy.wait()
            delta = lax.dot_general(
                high_held[:, part],
                low_held[...],
                (((0,), (0,)), ((), ())),
                preferred_element_type=jnp.float32,
            )
            kept = w_held[:, part].T.astype(jnp.float32)
            out_ref[part, :] = (kept + mix_rate * delta).astype(jnp.bfloat16)


def merged(*tasks):
    spans, operands, specs, shapes, scratch, copies = [], [], [], [], [], 0
    for task in tasks:
        if len(task) == 2:
            used = task[0].size // lanes
            tall = -(-used // sublanes) * sublanes
            spans.append(None)
            operands += [a.reshape(used, lanes) for a in task]
            specs += [in_vmem] * 2
            shapes.append(jax.ShapeDtypeStruct((tall, lanes), jnp.bfloat16))
            continue
        w, low, high, first, last = task
        rows, total, rank = w.shape[0], last - first, low.shape[1]
        block = 2 * lanes
        blocks = [min(block, total - base) for base in range(0, total, block)]
        spans.append((first, blocks))
        operands += [pltpu.with_memory_space_constraint(a, pltpu.HBM) for a in (w, low.T, high)]
        specs += [in_hbm] * 3
        shapes.append(jax.ShapeDtypeStruct((total, rows), jnp.bfloat16))
        scratch += [
            pltpu.VMEM((rows, total), jnp.bfloat16),
            pltpu.VMEM((rank, rows), jnp.bfloat16),
            pltpu.VMEM((rank, total), jnp.bfloat16),
        ]
        copies += 2 + len(blocks)
    return pl.pallas_call(
        functools.partial(merge_body, spans),
        in_specs=specs,
        out_specs=[in_vmem] * len(shapes),
        out_shape=shapes,
        scratch_shapes=[*scratch, pltpu.SemaphoreType.DMA((copies,))],
        compiler_params=pltpu.CompilerParams(vmem_limit_bytes=12 << 20),
    )(*operands)


def place_body(count, moves, outs_at, *refs):
    sems = refs[-1]
    me = lax.axis_index("shard")
    sign = 1 - 2 * lax.rem(me, 2)
    for act in ("start", "wait"):
        for j, (piece, (out, axis, extent, base, offset)) in enumerate(zip(refs, moves)):
            owner = me + sign * offset

            @pl.when(jnp.logical_and(owner >= 0, owner < count))
            def _():
                start = pl.multiple_of(owner * extent + base, (sublanes, lanes)[axis])
                where = [slice(None), slice(None)]
                where[axis] = pl.ds(start, piece.shape[axis])
                copy = pltpu.make_async_copy(piece, refs[outs_at + out].at[tuple(where)], sems.at[j])
                getattr(copy, act)()


def place(outs, pieces, count):
    targets = list(dict.fromkeys(piece[0] for piece in pieces))
    arrays = [piece[-1] for piece in pieces]
    moves = [(targets.index(piece[0]), *piece[1:-1]) for piece in pieces]
    shapes = []
    for target in targets:
        _, axis, extent, _, _, array = next(piece for piece in pieces if piece[0] == target)
        shape = list(array.shape)
        shape[axis] = count * extent
        shapes.append(jax.ShapeDtypeStruct(tuple(shape), jnp.bfloat16))
    kept = [outs[target] for target in targets if target in outs]
    placed = pl.pallas_call(
        functools.partial(place_body, count, moves, len(arrays) + len(kept)),
        in_specs=[in_vmem] * len(arrays) + [in_hbm] * len(kept),
        out_specs=[in_hbm] * len(targets),
        out_shape=shapes,
        scratch_shapes=[pltpu.SemaphoreType.DMA((len(arrays),))],
        input_output_aliases={len(arrays) + j: j for j in range(len(kept))},
        compiler_params=pltpu.CompilerParams(vmem_limit_bytes=4 << 20),
    )(*arrays, *kept)
    outs.update(zip(targets, placed))


def hops(count):
    plan = []
    for k in range(1, count):
        for name, source, parity in (("a", "b", 0), ("b", "a", 1)):
            pairs = []
            for i in range(parity, count - 1, 2):
                if i + k < count:
                    pairs.append((i + 1, i))
                if i + 1 - k >= 0:
                    pairs.append((i, i + 1))
            if pairs:
                offset = k if parity == 0 else -k
                plan.append((f"{name}{k}", f"{source}{k - 1}", pairs, offset))
    return plan


def pick_body(first_ref, second_ref, out_ref):
    leads = lax.axis_index("width") == 0

    @pl.when(leads)
    def _():
        out_ref[...] = first_ref[...]

    @pl.when(jnp.logical_not(leads))
    def _():
        out_ref[...] = second_ref[...]


def staggered(piece, pairs, cores):
    def of(chosen):
        return [(i * cores + core, j * cores + core) for i, j in pairs for core in chosen]

    first = lax.ppermute(piece, ("shard", "width"), of(range(1)))
    second = lax.ppermute(piece, ("shard", "width"), of(range(1, cores)))
    return pl.pallas_call(
        pick_body,
        in_specs=[in_vmem] * 2,
        out_specs=in_vmem,
        out_shape=jax.ShapeDtypeStruct(piece.shape, piece.dtype),
        compiler_params=pltpu.CompilerParams(vmem_limit_bytes=4 << 20),
    )(first, second)


head = 2 * lanes
chunk_names = ("mixed_head", "mixed_rest", "query", "norm", "key", "value")


def groups(count):
    whole = (chunk_names,)
    return [whole] * (count - 2) + [(chunk_names[:-2], chunk_names[-2:-1], chunk_names[-1:])]


def by_line(count, cores, query, key, value, mixed, norms):
    rows, columns = query[0].shape[0], mixed[0].shape[1]
    pieces = {}
    (pieces["mixed_head"],) = merged((*mixed, 0, head))
    (pieces["mixed_rest"],) = merged((*mixed, head, columns))
    pieces["query"], pieces["key"], pieces["value"], row = merged(
        *((*weight, 0, weight[0].shape[1]) for weight in (query, key, value)), norms
    )
    pieces["norm"] = lax.all_gather(row, "width", axis=0, tiled=True)
    where = {
        "mixed_head": ("mixed", 0, columns, 0),
        "mixed_rest": ("mixed", 0, columns, head),
        "query": ("query", 1, rows, 0),
        "norm": ("norm", 0, pieces["norm"].shape[0], 0),
        "key": ("key", 1, rows, 0),
        "value": ("value", 1, rows, 0),
    }
    plan = hops(count)
    outs = {}
    held = {name: {"a0": piece, "b0": piece} for name, piece in pieces.items()}
    arrived = {name: [(*where[name], 0, piece)] for name, piece in pieces.items()}
    for k, parts in enumerate(groups(count), start=1):
        for hop, source, pairs, offset in plan:
            if int(hop[1:]) == k:
                for name in chunk_names:
                    if (hop, name) == ("a1", "mixed_head"):
                        held[name][hop] = staggered(held[name][source], pairs, cores)
                    else:
                        held[name][hop] = lax.ppermute(held[name][source], "shard", pairs)
                    arrived[name].append((*where[name], offset, held[name][hop]))
        for part in parts:
            place(outs, [move for name in part for move in arrived[name]], count)
        arrived = {name: [] for name in chunk_names}
    used = norms[0].size // lanes
    serve_norm = outs["norm"].reshape(-1, row.shape[0], lanes)[:, :used].reshape(-1)
    return outs["query"], outs["key"], outs["value"], outs["mixed"], serve_norm


def by_gather(count, cores, query, key, value, mixed, norms):
    finals = []
    for axis, (w, low, high) in ((0, query), (0, key), (0, value), (1, mixed)):
        result = w.astype(jnp.float32) + mix_rate * jnp.dot(
            low, high, preferred_element_type=jnp.float32
        )
        narrow = result.astype(jnp.bfloat16)
        finals.append(lax.all_gather(narrow, "shard", axis=axis, tiled=True).T)
    norm = (norms[0] + norms[1]).astype(jnp.bfloat16)
    serve_norm = lax.all_gather(norm, ("shard", "width"), axis=0, tiled=True)
    return *finals, serve_norm


def on_device(form, count, cores, *args):
    weights = [args[3 * j : 3 * j + 3] for j in range(4)]
    return form(count, cores, *weights, args[12:])


def solution(mesh):
    column_cut = (P(("shift", "shard"), "width"), P(("shift", "shard"), None), P("shift", "width"))
    row_cut = (P(("shift", "width"), "shard"), P(("shift", "width"), None), P("shift", "shard"))
    norm = P(("shift", "shard", "width"))
    count, cores = mesh.shape["shard"], mesh.shape["width"]

    def step(*args):
        rows = args[0].shape[0] // (mesh.shape["shift"] * count)
        columns = args[9].shape[1] // count
        narrow = [args[j].shape[1] // cores for j in (0, 3, 6)]
        gains = args[12].shape[0] // (mesh.shape["shift"] * count * cores)
        aligned = all(size % (2 * lanes) == 0 for size in (rows, columns, *narrow, gains))
        line = count > 2 and cores > 1 and aligned and columns > head
        program = jax.shard_map(
            functools.partial(on_device, by_line if line else by_gather, count, cores),
            mesh=mesh,
            in_specs=(*column_cut, *column_cut, *column_cut, *row_cut, norm, norm),
            out_specs=(
                P(("shift", "width"), None),
                P(("shift", "width"), None),
                P(("shift", "width"), None),
                P("shift", "width"),
                P("shift"),
            ),
            check_vma=False,
        )
        return program(*args)

    return step
```

```python
import functools

import jax
import jax.numpy as jnp
from jax import lax
from jax.experimental import pallas as pl
from jax.experimental.pallas import tpu as pltpu
from jax.sharding import PartitionSpec as P


mix_rate = 0.5
lanes = 128
sublanes = 8


in_vmem = pl.BlockSpec(memory_space=pltpu.VMEM)
in_hbm = pl.BlockSpec(memory_space=pltpu.HBM)


def merge_into(out_ref, first, w_ref, low_ref, high_ref, w_held, low_held, high_held, sems):
    total = out_ref.shape[0]
    copies = [
        pltpu.make_async_copy(low_ref, low_held, sems.at[0]),
        pltpu.make_async_copy(high_ref.at[:, pl.ds(first, total)], high_held, sems.at[1]),
    ]
    parts = [pl.ds(base, size) for base, size in blocks(total)]
    for j, (base, size) in enumerate(blocks(total)):
        source = w_ref.at[:, pl.ds(first + base, size)]
        copies.append(pltpu.make_async_copy(source, w_held.at[:, parts[j]], sems.at[2 + j]))
    for copy in copies:
        copy.start()

    def finish():
        copies[0].wait()
        copies[1].wait()
        for part, copy in zip(parts, copies[2:]):
            copy.wait()
            delta = lax.dot_general(
                high_held[:, part],
                low_held[...],
                (((0,), (0,)), ((), ())),
                preferred_element_type=jnp.float32,
            )
            kept = w_held[:, part].T.astype(jnp.float32)
            out_ref[part, :] = (kept + mix_rate * delta).astype(jnp.bfloat16)

    return finish


def blocks(total):
    size = 2 * lanes
    return [(base, min(size, total - base)) for base in range(0, total, size)]


def scratch_of(w, low, total):
    rows, rank = w.shape[0], low.shape[1]
    return [
        pltpu.VMEM((rows, total), jnp.bfloat16),
        pltpu.VMEM((rank, rows), jnp.bfloat16),
        pltpu.VMEM((rank, total), jnp.bfloat16),
        pltpu.SemaphoreType.DMA((2 + len(blocks(total)),)),
    ]


def operands_of(w, low, high):
    return [pltpu.with_memory_space_constraint(a, pltpu.HBM) for a in (w, low.T, high)]


merge_params = pltpu.CompilerParams(vmem_limit_bytes=12 << 20)


def leads():
    return lax.axis_index("width") == 0


def merged_head(w, low, high, head):
    rows, columns = w.shape

    def body(w_ref, low_ref, high_ref, head_ref, rest_ref, *scratch):
        merge_into(head_ref, 0, w_ref, low_ref, high_ref, *scratch[:4])()

        @pl.when(jnp.logical_not(leads()))
        def _():
            merge_into(rest_ref, head, w_ref, low_ref, high_ref, *scratch[4:])()

    return pl.pallas_call(
        body,
        in_specs=[in_hbm] * 3,
        out_specs=[in_vmem] * 2,
        out_shape=[jax.ShapeDtypeStruct((n, rows), jnp.bfloat16) for n in (head, columns - head)],
        scratch_shapes=scratch_of(w, low, head) + scratch_of(w, low, columns - head),
        compiler_params=merge_params,
    )(*operands_of(w, low, high))


def merged_rest(rest, w, low, high, head):
    def body(w_ref, low_ref, high_ref, _, rest_ref, *scratch):
        @pl.when(leads())
        def _():
            merge_into(rest_ref, head, w_ref, low_ref, high_ref, *scratch)()

    return pl.pallas_call(
        body,
        in_specs=[in_hbm] * 3 + [in_vmem],
        out_specs=in_vmem,
        out_shape=jax.ShapeDtypeStruct(rest.shape, rest.dtype),
        scratch_shapes=scratch_of(w, low, rest.shape[0]),
        input_output_aliases={3: 0},
        compiler_params=merge_params,
    )(*operands_of(w, low, high), rest)


def merged_others(weights, norms):
    used = norms[0].size // lanes
    tall = -(-used // sublanes) * sublanes
    count = len(weights)

    def body(*refs):
        inputs, (train_ref, step_ref) = refs[: 3 * count], refs[3 * count : 3 * count + 2]
        outs, row_ref = refs[3 * count + 2 :][:count], refs[4 * count + 2]
        scratch = refs[4 * count + 3 :]
        finishes = [
            merge_into(outs[j], 0, *inputs[3 * j : 3 * j + 3], *scratch[4 * j : 4 * j + 4])
            for j in range(count)
        ]
        row_ref[...] = jnp.zeros_like(row_ref)
        row_ref[:used, :] = (train_ref[...] + step_ref[...]).astype(jnp.bfloat16)
        for finish in finishes:
            finish()

    shapes = [jax.ShapeDtypeStruct(w.shape[::-1], jnp.bfloat16) for w, _, _ in weights]
    return pl.pallas_call(
        body,
        in_specs=[in_hbm] * (3 * count) + [in_vmem] * 2,
        out_specs=[in_vmem] * (count + 1),
        out_shape=[*shapes, jax.ShapeDtypeStruct((tall, lanes), jnp.bfloat16)],
        scratch_shapes=[ref for w, low, _ in weights for ref in scratch_of(w, low, w.shape[1])],
        compiler_params=merge_params,
    )(*(a for weight in weights for a in operands_of(*weight)), *(a.reshape(used, lanes) for a in norms))


def place_body(count, moves, outs_at, *refs):
    sems = refs[-1]
    me = lax.axis_index("shard")
    sign = 1 - 2 * lax.rem(me, 2)
    for act in ("start", "wait"):
        for j, (piece, (out, axis, extent, base, offset)) in enumerate(zip(refs, moves)):
            owner = me + sign * offset

            @pl.when(jnp.logical_and(owner >= 0, owner < count))
            def _():
                start = pl.multiple_of(owner * extent + base, (sublanes, lanes)[axis])
                where = [slice(None), slice(None)]
                where[axis] = pl.ds(start, piece.shape[axis])
                copy = pltpu.make_async_copy(piece, refs[outs_at + out].at[tuple(where)], sems.at[j])
                getattr(copy, act)()


def place(outs, pieces, count):
    targets = list(dict.fromkeys(piece[0] for piece in pieces))
    arrays = [piece[-1] for piece in pieces]
    moves = [(targets.index(piece[0]), *piece[1:-1]) for piece in pieces]
    shapes = []
    for target in targets:
        _, axis, extent, _, _, array = next(piece for piece in pieces if piece[0] == target)
        shape = list(array.shape)
        shape[axis] = count * extent
        shapes.append(jax.ShapeDtypeStruct(tuple(shape), jnp.bfloat16))
    kept = [outs[target] for target in targets if target in outs]
    placed = pl.pallas_call(
        functools.partial(place_body, count, moves, len(arrays) + len(kept)),
        in_specs=[in_vmem] * len(arrays) + [in_hbm] * len(kept),
        out_specs=[in_hbm] * len(targets),
        out_shape=shapes,
        scratch_shapes=[pltpu.SemaphoreType.DMA((len(arrays),))],
        input_output_aliases={len(arrays) + j: j for j in range(len(kept))},
        compiler_params=pltpu.CompilerParams(vmem_limit_bytes=4 << 20),
    )(*arrays, *kept)
    outs.update(zip(targets, placed))


def hops(count):
    plan = []
    for k in range(1, count):
        for name, source, parity in (("a", "b", 0), ("b", "a", 1)):
            pairs = []
            for i in range(parity, count - 1, 2):
                if i + k < count:
                    pairs.append((i + 1, i))
                if i + 1 - k >= 0:
                    pairs.append((i, i + 1))
            if pairs:
                offset = k if parity == 0 else -k
                plan.append((f"{name}{k}", f"{source}{k - 1}", pairs, offset))
    return plan


head = lanes
chunk_names = ("mixed_head", "mixed_rest", "query", "norm", "key", "value")


def groups(count):
    whole = (chunk_names,)
    return [whole] * (count - 2) + [(chunk_names[:-2], chunk_names[-2:-1], chunk_names[-1:])]


def by_line(count, query, key, value, mixed, norms):
    rows, columns = query[0].shape[0], mixed[0].shape[1]
    pieces = {}
    pieces["mixed_head"], rest = merged_head(*mixed, head)
    pieces["mixed_rest"] = merged_rest(rest, *mixed, head)
    pieces["query"], pieces["key"], pieces["value"], row = merged_others((query, key, value), norms)
    pieces["norm"] = lax.all_gather(row, "width", axis=0, tiled=True)
    where = {
        "mixed_head": ("mixed", 0, columns, 0),
        "mixed_rest": ("mixed", 0, columns, head),
        "query": ("query", 1, rows, 0),
        "norm": ("norm", 0, pieces["norm"].shape[0], 0),
        "key": ("key", 1, rows, 0),
        "value": ("value", 1, rows, 0),
    }
    plan = hops(count)
    outs = {}
    held = {name: {"a0": piece, "b0": piece} for name, piece in pieces.items()}
    arrived = {name: [(*where[name], 0, piece)] for name, piece in pieces.items()}
    for k, parts in enumerate(groups(count), start=1):
        for hop, source, pairs, offset in plan:
            if int(hop[1:]) == k:
                for name in chunk_names:
                    held[name][hop] = lax.ppermute(held[name][source], "shard", pairs)
                    arrived[name].append((*where[name], offset, held[name][hop]))
        for part in parts:
            place(outs, [move for name in part for move in arrived[name]], count)
        arrived = {name: [] for name in chunk_names}
    used = norms[0].size // lanes
    serve_norm = outs["norm"].reshape(-1, row.shape[0], lanes)[:, :used].reshape(-1)
    return outs["query"], outs["key"], outs["value"], outs["mixed"], serve_norm


def by_gather(count, query, key, value, mixed, norms):
    finals = []
    for axis, (w, low, high) in ((0, query), (0, key), (0, value), (1, mixed)):
        result = w.astype(jnp.float32) + mix_rate * jnp.dot(
            low, high, preferred_element_type=jnp.float32
        )
        narrow = result.astype(jnp.bfloat16)
        finals.append(lax.all_gather(narrow, "shard", axis=axis, tiled=True).T)
    norm = (norms[0] + norms[1]).astype(jnp.bfloat16)
    serve_norm = lax.all_gather(norm, ("shard", "width"), axis=0, tiled=True)
    return *finals, serve_norm


def on_device(form, count, *args):
    weights = [args[3 * j : 3 * j + 3] for j in range(4)]
    return form(count, *weights, args[12:])


def solution(mesh):
    column_cut = (P(("shift", "shard"), "width"), P(("shift", "shard"), None), P("shift", "width"))
    row_cut = (P(("shift", "width"), "shard"), P(("shift", "width"), None), P("shift", "shard"))
    norm = P(("shift", "shard", "width"))
    count = mesh.shape["shard"]

    def step(*args):
        rows = args[0].shape[0] // (mesh.shape["shift"] * count)
        columns = args[9].shape[1] // count
        narrow = [args[j].shape[1] // mesh.shape["width"] for j in (0, 3, 6)]
        gains = args[12].shape[0] // (mesh.shape["shift"] * count * mesh.shape["width"])
        aligned = all(size % (2 * lanes) == 0 for size in (rows, columns, *narrow, gains))
        line = count > 2 and aligned
        program = jax.shard_map(
            functools.partial(on_device, by_line if line else by_gather, count),
            mesh=mesh,
            in_specs=(*column_cut, *column_cut, *column_cut, *row_cut, norm, norm),
            out_specs=(
                P(("shift", "width"), None),
                P(("shift", "width"), None),
                P(("shift", "width"), None),
                P("shift", "width"),
                P("shift"),
            ),
            check_vma=False,
        )
        return program(*args)

    return step
```

```python
import functools

import jax
import jax.numpy as jnp
from jax import lax
from jax.experimental import pallas as pl
from jax.experimental.pallas import tpu as pltpu
from jax.sharding import PartitionSpec as P


mix_rate = 0.5
lanes = 128
sublanes = 8


in_vmem = pl.BlockSpec(memory_space=pltpu.VMEM)
in_hbm = pl.BlockSpec(memory_space=pltpu.HBM)


def blocks(total):
    size = 2 * lanes
    return [(base, min(size, total - base)) for base in range(0, total, size)]


def merge_into(out_ref, offset, total, first, w_ref, low_ref, high_ref, w_held, low_held, high_held, sems):
    copies = [
        pltpu.make_async_copy(low_ref, low_held, sems.at[0]),
        pltpu.make_async_copy(high_ref.at[:, pl.ds(first, total)], high_held, sems.at[1]),
    ]
    for j, (base, size) in enumerate(blocks(total)):
        source, target = w_ref.at[:, pl.ds(first + base, size)], w_held.at[:, pl.ds(base, size)]
        copies.append(pltpu.make_async_copy(source, target, sems.at[2 + j]))
    for copy in copies:
        copy.start()

    def finish():
        copies[0].wait()
        copies[1].wait()
        width = out_ref.shape[1]
        for (base, size), copy in zip(blocks(total), copies[2:]):
            copy.wait()
            part = pl.ds(base, size)
            delta = lax.dot_general(
                high_held[:, part],
                low_held[...],
                (((0,), (0,)), ((), ())),
                preferred_element_type=jnp.float32,
            )
            kept = w_held[:, part].T.astype(jnp.float32)
            result = (kept + mix_rate * delta).astype(jnp.bfloat16)
            for h in range(w_held.shape[0] // width):
                row = offset + h * total + base
                out_ref[pl.ds(row, size), :] = result[:, h * width : (h + 1) * width]

    return finish


def scratch_of(w, low, total):
    rows, rank = w.shape[0], low.shape[1]
    return [
        pltpu.VMEM((rows, total), jnp.bfloat16),
        pltpu.VMEM((rank, rows), jnp.bfloat16),
        pltpu.VMEM((rank, total), jnp.bfloat16),
        pltpu.SemaphoreType.DMA((2 + len(blocks(total)),)),
    ]


def hbm(*arrays):
    return [pltpu.with_memory_space_constraint(a, pltpu.HBM) for a in arrays]


def tiles(rows):
    return -(-rows // sublanes) * sublanes


merge_params = pltpu.CompilerParams(vmem_limit_bytes=12 << 20)


def merged_head(w, low, high, head):
    def body(w_ref, low_ref, high_ref, out_ref, *scratch):
        merge_into(out_ref, 0, head, 0, w_ref, low_ref, high_ref, *scratch)()

    return pl.pallas_call(
        body,
        in_specs=[in_hbm] * 3,
        out_specs=in_vmem,
        out_shape=jax.ShapeDtypeStruct((head, w.shape[0]), jnp.bfloat16),
        scratch_shapes=scratch_of(w, low, head),
        compiler_params=merge_params,
    )(*hbm(w, low.T, high))


def merged_body(mixed, query, norms, head):
    rest = mixed[0].shape[1] - head
    width = query[0].shape[0]
    below = rest * (mixed[0].shape[0] // width)
    used = norms[0].size // lanes
    held = 4

    def body(wm, lm, hm, wq, lq, hq, train, step, out_ref, row_ref, *scratch):
        finish_mixed = merge_into(out_ref, 0, rest, head, wm, lm, hm, *scratch[:held])
        finish_query = merge_into(
            out_ref, below, wq.shape[1], 0, wq, lq, hq, *scratch[held : 2 * held]
        )
        train_held, step_held, sems = scratch[2 * held :]
        copies = [
            pltpu.make_async_copy(train, train_held, sems.at[0]),
            pltpu.make_async_copy(step, step_held, sems.at[1]),
        ]
        for copy in copies:
            copy.start()
        finish_mixed()
        finish_query()
        for copy in copies:
            copy.wait()
        row_ref[...] = jnp.zeros_like(row_ref)
        row_ref[:used, :] = (train_held[...] + step_held[...]).astype(jnp.bfloat16)

    return pl.pallas_call(
        body,
        in_specs=[in_hbm] * 8,
        out_specs=[in_vmem] * 2,
        out_shape=[
            jax.ShapeDtypeStruct((below + query[0].shape[1], width), jnp.bfloat16),
            jax.ShapeDtypeStruct((tiles(used), lanes), jnp.bfloat16),
        ],
        scratch_shapes=[
            *scratch_of(mixed[0], mixed[1], rest),
            *scratch_of(query[0], query[1], query[0].shape[1]),
            *[pltpu.VMEM((used, lanes), jnp.float32)] * 2,
            pltpu.SemaphoreType.DMA((2,)),
        ],
        compiler_params=merge_params,
    )(
        *hbm(mixed[0], mixed[1].T, mixed[2], query[0], query[1].T, query[2]),
        *hbm(*(a.reshape(used, lanes) for a in norms)),
    )


def merged_tail(key, value, rows_of_cores, cores, used):
    under = key[0].shape[1] * (key[0].shape[0] // lanes)
    packed = tiles(cores * used)
    held = 4

    def body(wk, lk, hk, wv, lv, hv, rows_ref, key_ref, value_ref, *scratch):
        finish_key = merge_into(key_ref, 0, wk.shape[1], 0, wk, lk, hk, *scratch[:held])
        finish_value = merge_into(value_ref, 0, wv.shape[1], 0, wv, lv, hv, *scratch[held : 2 * held])
        packed_ref = scratch[2 * held]
        packed_ref[...] = jnp.zeros_like(packed_ref)
        rows = rows_ref[...].astype(jnp.float32)
        tall = rows.shape[0] // cores
        for core in range(cores):
            packed_ref[core * used : (core + 1) * used, :] = rows[core * tall : core * tall + used]
        key_ref[pl.ds(under, packed), :] = packed_ref[...].astype(jnp.bfloat16)
        finish_key()
        finish_value()

    return pl.pallas_call(
        body,
        in_specs=[in_hbm] * 6 + [in_vmem],
        out_specs=[in_vmem] * 2,
        out_shape=[
            jax.ShapeDtypeStruct((under + packed, lanes), jnp.bfloat16),
            jax.ShapeDtypeStruct(value[0].shape[::-1], jnp.bfloat16),
        ],
        scratch_shapes=[
            *scratch_of(key[0], key[1], key[0].shape[1]),
            *scratch_of(value[0], value[1], value[0].shape[1]),
            pltpu.VMEM((packed, lanes), jnp.float32),
        ],
        compiler_params=merge_params,
    )(*hbm(key[0], key[1].T, key[2], value[0], value[1].T, value[2]), rows_of_cores)


def place_body(count, moves, pieces_at, outs_at, *refs):
    sems = refs[-1]
    me = lax.axis_index("shard")
    sign = 1 - 2 * lax.rem(me, 2)
    for act in ("start", "wait"):
        for j, (piece, out, low, rows, tall, down, wide, right, offset) in enumerate(moves):
            owner = me + sign * offset

            @pl.when(jnp.logical_and(owner >= 0, owner < count))
            def _():
                source = refs[pieces_at + piece].at[pl.ds(low, rows)]
                row = pl.multiple_of(owner * tall + down, sublanes)
                column = pl.multiple_of(owner * wide + right, lanes)
                target = refs[outs_at + out].at[pl.ds(row, rows), pl.ds(column, source.shape[1])]
                getattr(pltpu.make_async_copy(source, target, sems.at[j]), act)()


def place(outs, shapes, pieces, count):
    targets = list(dict.fromkeys(region[0] for regions, _, _ in pieces for region in regions))
    arrays = [array for _, _, array in pieces]
    moves = [
        (j, targets.index(region[0]), *region[1:], offset)
        for j, (regions, offset, _) in enumerate(pieces)
        for region in regions
    ]
    kept = [outs[target] for target in targets if target in outs]
    placed = pl.pallas_call(
        functools.partial(place_body, count, moves, 0, len(arrays) + len(kept)),
        in_specs=[in_vmem] * len(arrays) + [in_hbm] * len(kept),
        out_specs=[in_hbm] * len(targets),
        out_shape=[jax.ShapeDtypeStruct(shapes[target], jnp.bfloat16) for target in targets],
        scratch_shapes=[pltpu.SemaphoreType.DMA((len(moves),))],
        input_output_aliases={len(arrays) + j: j for j in range(len(kept))},
        compiler_params=pltpu.CompilerParams(vmem_limit_bytes=4 << 20),
    )(*arrays, *kept)
    outs.update(zip(targets, placed))


def hops(count):
    plan = []
    for k in range(1, count):
        for name, source, parity in (("a", "b", 0), ("b", "a", 1)):
            pairs = []
            for i in range(parity, count - 1, 2):
                if i + k < count:
                    pairs.append((i + 1, i))
                if i + 1 - k >= 0:
                    pairs.append((i, i + 1))
            if pairs:
                offset = k if parity == 0 else -k
                plan.append((f"{name}{k}", f"{source}{k - 1}", pairs, offset))
    return plan


head = lanes
chunk_names = ("head", "body", "key", "value")


def groups(count):
    whole = (chunk_names,)
    return [whole] * (count - 2) + [(chunk_names[:-2], chunk_names[-2:-1], chunk_names[-1:])]


def by_line(count, cores, query, key, value, mixed, norms):
    rows, columns = query[0].shape[0], mixed[0].shape[1]
    used = norms[0].size // lanes
    packed = tiles(cores * used)
    pieces = {}
    pieces["head"] = merged_head(*mixed, head)
    pieces["body"], row = merged_body(mixed, query, norms, head)
    rows_of_cores = lax.all_gather(row, "width", axis=0, tiled=True)
    pieces["key"], pieces["value"] = merged_tail(key, value, rows_of_cores, cores, used)
    rest, halves = columns - head, mixed[0].shape[0] // rows
    wide = {name: weight[0].shape[1] for name, weight in (("query", query), ("key", key), ("value", value))}
    regions = {
        "head": [("mixed", 0, head, columns, 0, 0, 0)],
        "body": [("mixed", h * rest, rest, columns, head, 0, h * rows) for h in range(halves)]
        + [("query", halves * rest, wide["query"], 0, 0, rows, 0)],
        "key": [("key", b * wide["key"], wide["key"], 0, 0, rows, b * lanes) for b in range(rows // lanes)]
        + [("norm", wide["key"] * (rows // lanes), packed, packed, 0, 0, 0)],
        "value": [("value", 0, wide["value"], 0, 0, rows, 0)],
    }
    shapes = {name: (size, count * rows) for name, size in wide.items()}
    shapes["mixed"] = (count * columns, mixed[0].shape[0])
    shapes["norm"] = (count * packed, lanes)
    plan = hops(count)
    outs = {}
    held = {name: {"a0": piece, "b0": piece} for name, piece in pieces.items()}
    arrived = {name: [(regions[name], 0, piece)] for name, piece in pieces.items()}
    for k, parts in enumerate(groups(count), start=1):
        for hop, source, pairs, offset in plan:
            if int(hop[1:]) == k:
                for name in chunk_names:
                    held[name][hop] = lax.ppermute(held[name][source], "shard", pairs)
                    arrived[name].append((regions[name], offset, held[name][hop]))
        for part in parts:
            place(outs, shapes, [piece for name in part for piece in arrived[name]], count)
        arrived = {name: [] for name in chunk_names}
    serve_norm = outs["norm"].reshape(count, packed, lanes)[:, : cores * used].reshape(-1)
    return outs["query"], outs["key"], outs["value"], outs["mixed"], serve_norm


def by_gather(count, cores, query, key, value, mixed, norms):
    finals = []
    for axis, (w, low, high) in ((0, query), (0, key), (0, value), (1, mixed)):
        result = w.astype(jnp.float32) + mix_rate * jnp.dot(
            low, high, preferred_element_type=jnp.float32
        )
        narrow = result.astype(jnp.bfloat16)
        finals.append(lax.all_gather(narrow, "shard", axis=axis, tiled=True).T)
    norm = (norms[0] + norms[1]).astype(jnp.bfloat16)
    serve_norm = lax.all_gather(norm, ("shard", "width"), axis=0, tiled=True)
    return *finals, serve_norm


def on_device(form, count, cores, *args):
    weights = [args[3 * j : 3 * j + 3] for j in range(4)]
    return form(count, cores, *weights, args[12:])


def solution(mesh):
    column_cut = (P(("shift", "shard"), "width"), P(("shift", "shard"), None), P("shift", "width"))
    row_cut = (P(("shift", "width"), "shard"), P(("shift", "width"), None), P("shift", "shard"))
    norm = P(("shift", "shard", "width"))
    count, cores = mesh.shape["shard"], mesh.shape["width"]

    def step(*args):
        rows = args[0].shape[0] // (mesh.shape["shift"] * count)
        columns = args[9].shape[1] // count
        narrow = [args[j].shape[1] // cores for j in (0, 3, 6)]
        gains = args[12].shape[0] // (mesh.shape["shift"] * count * cores)
        aligned = all(size % (2 * lanes) == 0 for size in (rows, columns, *narrow, gains))
        tall = args[9].shape[0] // (mesh.shape["shift"] * cores)
        line = count > 2 and aligned and tall % rows == 0
        program = jax.shard_map(
            functools.partial(on_device, by_line if line else by_gather, count, cores),
            mesh=mesh,
            in_specs=(*column_cut, *column_cut, *column_cut, *row_cut, norm, norm),
            out_specs=(
                P(("shift", "width"), None),
                P(("shift", "width"), None),
                P(("shift", "width"), None),
                P("shift", "width"),
                P("shift"),
            ),
            check_vma=False,
        )
        return program(*args)

    return step
```

```python
import functools

import jax
import jax.numpy as jnp
from jax import lax
from jax.experimental import pallas as pl
from jax.experimental.pallas import tpu as pltpu
from jax.sharding import PartitionSpec as P


mix_rate = 0.5
lanes = 128
sublanes = 8


in_vmem = pl.BlockSpec(memory_space=pltpu.VMEM)
in_hbm = pl.BlockSpec(memory_space=pltpu.HBM)


def blocks(total):
    size = 2 * lanes
    return [(base, min(size, total - base)) for base in range(0, total, size)]


def merge_into(out_ref, offset, total, first, w_ref, low_ref, high_ref, w_held, low_held, high_held, sems):
    copies = [
        pltpu.make_async_copy(low_ref, low_held, sems.at[0]),
        pltpu.make_async_copy(high_ref.at[:, pl.ds(first, total)], high_held, sems.at[1]),
    ]
    for j, (base, size) in enumerate(blocks(total)):
        source, target = w_ref.at[:, pl.ds(first + base, size)], w_held.at[:, pl.ds(base, size)]
        copies.append(pltpu.make_async_copy(source, target, sems.at[2 + j]))
    for copy in copies:
        copy.start()

    def finish():
        copies[0].wait()
        copies[1].wait()
        width = out_ref.shape[1]
        for (base, size), copy in zip(blocks(total), copies[2:]):
            copy.wait()
            part = pl.ds(base, size)
            delta = lax.dot_general(
                high_held[:, part],
                low_held[...],
                (((0,), (0,)), ((), ())),
                preferred_element_type=jnp.float32,
            )
            kept = w_held[:, part].T.astype(jnp.float32)
            result = (kept + mix_rate * delta).astype(jnp.bfloat16)
            for h in range(w_held.shape[0] // width):
                row = offset + h * total + base
                out_ref[pl.ds(row, size), :] = result[:, h * width : (h + 1) * width]

    return finish


def scratch_of(w, low, total):
    rows, rank = w.shape[0], low.shape[1]
    return [
        pltpu.VMEM((rows, total), jnp.bfloat16),
        pltpu.VMEM((rank, rows), jnp.bfloat16),
        pltpu.VMEM((rank, total), jnp.bfloat16),
        pltpu.SemaphoreType.DMA((2 + len(blocks(total)),)),
    ]


def hbm(*arrays):
    return [pltpu.with_memory_space_constraint(a, pltpu.HBM) for a in arrays]


def tiles(rows):
    return -(-rows // sublanes) * sublanes


merge_params = pltpu.CompilerParams(vmem_limit_bytes=12 << 20)


def merged_head(w, low, high, head):
    rows, rank = w.shape[0], low.shape[1]
    count = 4 if rows % (4 * lanes) == 0 else 1
    parts = [pl.ds(j * (rows // count), rows // count) for j in range(count)]
    ahead = pl.ds(0, head)

    def body(w_ref, low_ref, high_ref, out_ref, w_held, low_held, high_held, sems):
        copies = [
            pltpu.make_async_copy(w_ref.at[part, ahead], w_held.at[part], sems.at[j])
            for j, part in enumerate(parts)
        ]
        copies.append(pltpu.make_async_copy(low_ref, low_held, sems.at[count]))
        copies.append(pltpu.make_async_copy(high_ref.at[:, ahead], high_held, sems.at[count + 1]))
        for copy in copies:
            copy.start()
        copies[-1].wait()
        copies[-2].wait()
        for part, copy in zip(parts, copies):
            delta = lax.dot_general(
                high_held[...],
                low_held[:, part],
                (((0,), (0,)), ((), ())),
                preferred_element_type=jnp.float32,
            )
            copy.wait()
            kept = w_held[part, :].T.astype(jnp.float32)
            out_ref[:, part] = (kept + mix_rate * delta).astype(jnp.bfloat16)

    return pl.pallas_call(
        body,
        in_specs=[in_hbm] * 3,
        out_specs=in_vmem,
        out_shape=jax.ShapeDtypeStruct((head, rows), jnp.bfloat16),
        scratch_shapes=[
            pltpu.VMEM((rows, head), jnp.bfloat16),
            pltpu.VMEM((rank, rows), jnp.bfloat16),
            pltpu.VMEM((rank, head), jnp.bfloat16),
            pltpu.SemaphoreType.DMA((count + 2,)),
        ],
        compiler_params=merge_params,
    )(*hbm(w, low.T, high))


def merged_body(mixed, query, norms, head):
    rest = mixed[0].shape[1] - head
    width = query[0].shape[0]
    below = rest * (mixed[0].shape[0] // width)
    used = norms[0].size // lanes
    held = 4

    def body(wm, lm, hm, wq, lq, hq, train, step, out_ref, row_ref, *scratch):
        finish_mixed = merge_into(out_ref, 0, rest, head, wm, lm, hm, *scratch[:held])
        finish_query = merge_into(
            out_ref, below, wq.shape[1], 0, wq, lq, hq, *scratch[held : 2 * held]
        )
        train_held, step_held, sems = scratch[2 * held :]
        copies = [
            pltpu.make_async_copy(train, train_held, sems.at[0]),
            pltpu.make_async_copy(step, step_held, sems.at[1]),
        ]
        for copy in copies:
            copy.start()
        finish_mixed()
        finish_query()
        for copy in copies:
            copy.wait()
        row_ref[...] = jnp.zeros_like(row_ref)
        row_ref[:used, :] = (train_held[...] + step_held[...]).astype(jnp.bfloat16)

    return pl.pallas_call(
        body,
        in_specs=[in_hbm] * 8,
        out_specs=[in_vmem] * 2,
        out_shape=[
            jax.ShapeDtypeStruct((below + query[0].shape[1], width), jnp.bfloat16),
            jax.ShapeDtypeStruct((tiles(used), lanes), jnp.bfloat16),
        ],
        scratch_shapes=[
            *scratch_of(mixed[0], mixed[1], rest),
            *scratch_of(query[0], query[1], query[0].shape[1]),
            *[pltpu.VMEM((used, lanes), jnp.float32)] * 2,
            pltpu.SemaphoreType.DMA((2,)),
        ],
        compiler_params=merge_params,
    )(
        *hbm(mixed[0], mixed[1].T, mixed[2], query[0], query[1].T, query[2]),
        *hbm(*(a.reshape(used, lanes) for a in norms)),
    )


def merged_tail(key, value, rows_of_cores, cores, used):
    under = key[0].shape[1] * (key[0].shape[0] // lanes)
    packed = tiles(cores * used)
    held = 4

    def body(wk, lk, hk, wv, lv, hv, rows_ref, key_ref, value_ref, *scratch):
        finish_key = merge_into(key_ref, 0, wk.shape[1], 0, wk, lk, hk, *scratch[:held])
        finish_value = merge_into(value_ref, 0, wv.shape[1], 0, wv, lv, hv, *scratch[held : 2 * held])
        packed_ref = scratch[2 * held]
        packed_ref[...] = jnp.zeros_like(packed_ref)
        rows = rows_ref[...].astype(jnp.float32)
        tall = rows.shape[0] // cores
        for core in range(cores):
            packed_ref[core * used : (core + 1) * used, :] = rows[core * tall : core * tall + used]
        key_ref[pl.ds(under, packed), :] = packed_ref[...].astype(jnp.bfloat16)
        finish_key()
        finish_value()

    return pl.pallas_call(
        body,
        in_specs=[in_hbm] * 6 + [in_vmem],
        out_specs=[in_vmem] * 2,
        out_shape=[
            jax.ShapeDtypeStruct((under + packed, lanes), jnp.bfloat16),
            jax.ShapeDtypeStruct(value[0].shape[::-1], jnp.bfloat16),
        ],
        scratch_shapes=[
            *scratch_of(key[0], key[1], key[0].shape[1]),
            *scratch_of(value[0], value[1], value[0].shape[1]),
            pltpu.VMEM((packed, lanes), jnp.float32),
        ],
        compiler_params=merge_params,
    )(*hbm(key[0], key[1].T, key[2], value[0], value[1].T, value[2]), rows_of_cores)


def place_body(count, moves, pieces_at, outs_at, *refs):
    sems = refs[-1]
    me = lax.axis_index("shard")
    sign = 1 - 2 * lax.rem(me, 2)
    for act in ("start", "wait"):
        for j, (piece, out, low, rows, tall, down, wide, right, offset) in enumerate(moves):
            owner = me + sign * offset

            @pl.when(jnp.logical_and(owner >= 0, owner < count))
            def _():
                source = refs[pieces_at + piece].at[pl.ds(low, rows)]
                row = pl.multiple_of(owner * tall + down, sublanes)
                column = pl.multiple_of(owner * wide + right, lanes)
                target = refs[outs_at + out].at[pl.ds(row, rows), pl.ds(column, source.shape[1])]
                getattr(pltpu.make_async_copy(source, target, sems.at[j]), act)()


def place(outs, shapes, pieces, count):
    targets = list(dict.fromkeys(region[0] for regions, _, _ in pieces for region in regions))
    arrays = [array for _, _, array in pieces]
    moves = [
        (j, targets.index(region[0]), *region[1:], offset)
        for j, (regions, offset, _) in enumerate(pieces)
        for region in regions
    ]
    kept = [outs[target] for target in targets if target in outs]
    placed = pl.pallas_call(
        functools.partial(place_body, count, moves, 0, len(arrays) + len(kept)),
        in_specs=[in_vmem] * len(arrays) + [in_hbm] * len(kept),
        out_specs=[in_hbm] * len(targets),
        out_shape=[jax.ShapeDtypeStruct(shapes[target], jnp.bfloat16) for target in targets],
        scratch_shapes=[pltpu.SemaphoreType.DMA((len(moves),))],
        input_output_aliases={len(arrays) + j: j for j in range(len(kept))},
        compiler_params=pltpu.CompilerParams(vmem_limit_bytes=4 << 20),
    )(*arrays, *kept)
    outs.update(zip(targets, placed))


def hops(count):
    plan = []
    for k in range(1, count):
        for name, source, parity in (("a", "b", 0), ("b", "a", 1)):
            pairs = []
            for i in range(parity, count - 1, 2):
                if i + k < count:
                    pairs.append((i + 1, i))
                if i + 1 - k >= 0:
                    pairs.append((i, i + 1))
            if pairs:
                offset = k if parity == 0 else -k
                plan.append((f"{name}{k}", f"{source}{k - 1}", pairs, offset))
    return plan


head = lanes
chunk_names = ("head", "body", "key", "value")


def groups(count):
    whole = (chunk_names,)
    return [whole] * (count - 2) + [(chunk_names[:-2], chunk_names[-2:-1], chunk_names[-1:])]


def by_line(count, cores, query, key, value, mixed, norms):
    rows, columns = query[0].shape[0], mixed[0].shape[1]
    used = norms[0].size // lanes
    packed = tiles(cores * used)
    pieces = {}
    pieces["head"] = merged_head(*mixed, head)
    pieces["body"], row = merged_body(mixed, query, norms, head)
    rows_of_cores = lax.all_gather(row, "width", axis=0, tiled=True)
    pieces["key"], pieces["value"] = merged_tail(key, value, rows_of_cores, cores, used)
    rest, halves = columns - head, mixed[0].shape[0] // rows
    wide = {name: weight[0].shape[1] for name, weight in (("query", query), ("key", key), ("value", value))}
    regions = {
        "head": [("mixed", 0, head, columns, 0, 0, 0)],
        "body": [("mixed", h * rest, rest, columns, head, 0, h * rows) for h in range(halves)]
        + [("query", halves * rest, wide["query"], 0, 0, rows, 0)],
        "key": [("key", b * wide["key"], wide["key"], 0, 0, rows, b * lanes) for b in range(rows // lanes)]
        + [("norm", wide["key"] * (rows // lanes), packed, packed, 0, 0, 0)],
        "value": [("value", 0, wide["value"], 0, 0, rows, 0)],
    }
    shapes = {name: (size, count * rows) for name, size in wide.items()}
    shapes["mixed"] = (count * columns, mixed[0].shape[0])
    shapes["norm"] = (count * packed, lanes)
    plan = hops(count)
    outs = {}
    held = {name: {"a0": piece, "b0": piece} for name, piece in pieces.items()}
    arrived = {name: [(regions[name], 0, piece)] for name, piece in pieces.items()}
    for k, parts in enumerate(groups(count), start=1):
        for hop, source, pairs, offset in plan:
            if int(hop[1:]) == k:
                for name in chunk_names:
                    held[name][hop] = lax.ppermute(held[name][source], "shard", pairs)
                    arrived[name].append((regions[name], offset, held[name][hop]))
        for part in parts:
            place(outs, shapes, [piece for name in part for piece in arrived[name]], count)
        arrived = {name: [] for name in chunk_names}
    serve_norm = outs["norm"].reshape(count, packed, lanes)[:, : cores * used].reshape(-1)
    return outs["query"], outs["key"], outs["value"], outs["mixed"], serve_norm


def by_gather(count, cores, query, key, value, mixed, norms):
    finals = []
    for axis, (w, low, high) in ((0, query), (0, key), (0, value), (1, mixed)):
        result = w.astype(jnp.float32) + mix_rate * jnp.dot(
            low, high, preferred_element_type=jnp.float32
        )
        narrow = result.astype(jnp.bfloat16)
        finals.append(lax.all_gather(narrow, "shard", axis=axis, tiled=True).T)
    norm = (norms[0] + norms[1]).astype(jnp.bfloat16)
    serve_norm = lax.all_gather(norm, ("shard", "width"), axis=0, tiled=True)
    return *finals, serve_norm


def on_device(form, count, cores, *args):
    weights = [args[3 * j : 3 * j + 3] for j in range(4)]
    return form(count, cores, *weights, args[12:])


def solution(mesh):
    column_cut = (P(("shift", "shard"), "width"), P(("shift", "shard"), None), P("shift", "width"))
    row_cut = (P(("shift", "width"), "shard"), P(("shift", "width"), None), P("shift", "shard"))
    norm = P(("shift", "shard", "width"))
    count, cores = mesh.shape["shard"], mesh.shape["width"]

    def step(*args):
        rows = args[0].shape[0] // (mesh.shape["shift"] * count)
        columns = args[9].shape[1] // count
        narrow = [args[j].shape[1] // cores for j in (0, 3, 6)]
        gains = args[12].shape[0] // (mesh.shape["shift"] * count * cores)
        aligned = all(size % (2 * lanes) == 0 for size in (rows, columns, *narrow, gains))
        tall = args[9].shape[0] // (mesh.shape["shift"] * cores)
        line = count > 2 and aligned and tall % rows == 0
        program = jax.shard_map(
            functools.partial(on_device, by_line if line else by_gather, count, cores),
            mesh=mesh,
            in_specs=(*column_cut, *column_cut, *column_cut, *row_cut, norm, norm),
            out_specs=(
                P(("shift", "width"), None),
                P(("shift", "width"), None),
                P(("shift", "width"), None),
                P("shift", "width"),
                P("shift"),
            ),
            check_vma=False,
        )
        return program(*args)

    return step
```

```python
import functools

import jax
import jax.numpy as jnp
from jax import lax
from jax.experimental import pallas as pl
from jax.experimental.pallas import tpu as pltpu
from jax.sharding import PartitionSpec as P


mix_rate = 0.5
lanes = 128
sublanes = 8


in_vmem = pl.BlockSpec(memory_space=pltpu.VMEM)
in_hbm = pl.BlockSpec(memory_space=pltpu.HBM)


def blocks(total):
    size = 2 * lanes
    return [(base, min(size, total - base)) for base in range(0, total, size)]


def merge_into(out_ref, offset, total, first, w_ref, low_ref, high_ref, w_held, low_held, high_held, sems):
    copies = [
        pltpu.make_async_copy(low_ref, low_held, sems.at[0]),
        pltpu.make_async_copy(high_ref.at[:, pl.ds(first, total)], high_held, sems.at[1]),
    ]
    for j, (base, size) in enumerate(blocks(total)):
        source, target = w_ref.at[:, pl.ds(first + base, size)], w_held.at[:, pl.ds(base, size)]
        copies.append(pltpu.make_async_copy(source, target, sems.at[2 + j]))
    for copy in copies:
        copy.start()

    def finish():
        copies[0].wait()
        copies[1].wait()
        width = out_ref.shape[1]
        for (base, size), copy in zip(blocks(total), copies[2:]):
            copy.wait()
            part = pl.ds(base, size)
            delta = lax.dot_general(
                high_held[:, part],
                low_held[...],
                (((0,), (0,)), ((), ())),
                preferred_element_type=jnp.float32,
            )
            kept = w_held[:, part].T.astype(jnp.float32)
            result = (kept + mix_rate * delta).astype(jnp.bfloat16)
            for h in range(w_held.shape[0] // width):
                row = offset + h * total + base
                out_ref[pl.ds(row, size), :] = result[:, h * width : (h + 1) * width]

    return finish


def scratch_of(w, low, total):
    rows, rank = w.shape[0], low.shape[1]
    return [
        pltpu.VMEM((rows, total), jnp.bfloat16),
        pltpu.VMEM((rank, rows), jnp.bfloat16),
        pltpu.VMEM((rank, total), jnp.bfloat16),
        pltpu.SemaphoreType.DMA((2 + len(blocks(total)),)),
    ]


def hbm(*arrays):
    return [pltpu.with_memory_space_constraint(a, pltpu.HBM) for a in arrays]


def tiles(rows):
    return -(-rows // sublanes) * sublanes


merge_params = pltpu.CompilerParams(vmem_limit_bytes=12 << 20)


def merged_head(w, low, high, head):
    ahead = pl.ds(0, head)

    def body(w_ref, low_ref, high_ref, out_ref, w_held, low_held, high_held, sems):
        copies = [
            pltpu.make_async_copy(w_ref.at[:, ahead], w_held, sems.at[0]),
            pltpu.make_async_copy(low_ref, low_held, sems.at[1]),
            pltpu.make_async_copy(high_ref.at[:, ahead], high_held, sems.at[2]),
        ]
        for copy in copies:
            copy.start()
        copies[1].wait()
        copies[2].wait()
        delta = lax.dot_general(
            high_held[...],
            low_held[...],
            (((0,), (0,)), ((), ())),
            preferred_element_type=jnp.float32,
        )
        copies[0].wait()
        kept = w_held[...].T.astype(jnp.float32)
        out_ref[...] = (kept + mix_rate * delta).astype(jnp.bfloat16)

    return pl.pallas_call(
        body,
        in_specs=[in_hbm] * 3,
        out_specs=in_vmem,
        out_shape=jax.ShapeDtypeStruct((head, w.shape[0]), jnp.bfloat16),
        scratch_shapes=scratch_of(w, low, head),
        compiler_params=merge_params,
    )(*hbm(w, low.T, high))


def merged_body(mixed, query, norms, head):
    rest = mixed[0].shape[1] - head
    width = query[0].shape[0]
    below = rest * (mixed[0].shape[0] // width)
    used = norms[0].size // lanes
    held = 4

    def body(wm, lm, hm, wq, lq, hq, train, step, out_ref, row_ref, *scratch):
        finish_mixed = merge_into(out_ref, 0, rest, head, wm, lm, hm, *scratch[:held])
        finish_query = merge_into(
            out_ref, below, wq.shape[1], 0, wq, lq, hq, *scratch[held : 2 * held]
        )
        train_held, step_held, sems = scratch[2 * held :]
        copies = [
            pltpu.make_async_copy(train, train_held, sems.at[0]),
            pltpu.make_async_copy(step, step_held, sems.at[1]),
        ]
        for copy in copies:
            copy.start()
        finish_mixed()
        finish_query()
        for copy in copies:
            copy.wait()
        row_ref[...] = jnp.zeros_like(row_ref)
        row_ref[:used, :] = (train_held[...] + step_held[...]).astype(jnp.bfloat16)

    return pl.pallas_call(
        body,
        in_specs=[in_hbm] * 8,
        out_specs=[in_vmem] * 2,
        out_shape=[
            jax.ShapeDtypeStruct((below + query[0].shape[1], width), jnp.bfloat16),
            jax.ShapeDtypeStruct((tiles(used), lanes), jnp.bfloat16),
        ],
        scratch_shapes=[
            *scratch_of(mixed[0], mixed[1], rest),
            *scratch_of(query[0], query[1], query[0].shape[1]),
            *[pltpu.VMEM((used, lanes), jnp.float32)] * 2,
            pltpu.SemaphoreType.DMA((2,)),
        ],
        compiler_params=merge_params,
    )(
        *hbm(mixed[0], mixed[1].T, mixed[2], query[0], query[1].T, query[2]),
        *hbm(*(a.reshape(used, lanes) for a in norms)),
    )


def merged_tail(key, value, rows_of_cores, cores, used):
    under = key[0].shape[1] * (key[0].shape[0] // lanes)
    packed = tiles(cores * used)
    held = 4

    def body(wk, lk, hk, wv, lv, hv, rows_ref, key_ref, value_ref, *scratch):
        finish_key = merge_into(key_ref, 0, wk.shape[1], 0, wk, lk, hk, *scratch[:held])
        finish_value = merge_into(value_ref, 0, wv.shape[1], 0, wv, lv, hv, *scratch[held : 2 * held])
        packed_ref = scratch[2 * held]
        packed_ref[...] = jnp.zeros_like(packed_ref)
        rows = rows_ref[...].astype(jnp.float32)
        tall = rows.shape[0] // cores
        for core in range(cores):
            packed_ref[core * used : (core + 1) * used, :] = rows[core * tall : core * tall + used]
        key_ref[pl.ds(under, packed), :] = packed_ref[...].astype(jnp.bfloat16)
        finish_key()
        finish_value()

    return pl.pallas_call(
        body,
        in_specs=[in_hbm] * 6 + [in_vmem],
        out_specs=[in_vmem] * 2,
        out_shape=[
            jax.ShapeDtypeStruct((under + packed, lanes), jnp.bfloat16),
            jax.ShapeDtypeStruct(value[0].shape[::-1], jnp.bfloat16),
        ],
        scratch_shapes=[
            *scratch_of(key[0], key[1], key[0].shape[1]),
            *scratch_of(value[0], value[1], value[0].shape[1]),
            pltpu.VMEM((packed, lanes), jnp.float32),
        ],
        compiler_params=merge_params,
    )(*hbm(key[0], key[1].T, key[2], value[0], value[1].T, value[2]), rows_of_cores)


def place_body(count, moves, pieces_at, outs_at, *refs):
    sems = refs[-1]
    me = lax.axis_index("shard")
    sign = 1 - 2 * lax.rem(me, 2)
    for act in ("start", "wait"):
        for j, (piece, out, low, rows, tall, down, wide, right, offset) in enumerate(moves):
            owner = me + sign * offset

            @pl.when(jnp.logical_and(owner >= 0, owner < count))
            def _():
                source = refs[pieces_at + piece].at[pl.ds(low, rows)]
                row = pl.multiple_of(owner * tall + down, sublanes)
                column = pl.multiple_of(owner * wide + right, lanes)
                target = refs[outs_at + out].at[pl.ds(row, rows), pl.ds(column, source.shape[1])]
                getattr(pltpu.make_async_copy(source, target, sems.at[j]), act)()


def place(outs, shapes, pieces, count):
    targets = list(dict.fromkeys(region[0] for regions, _, _ in pieces for region in regions))
    arrays = [array for _, _, array in pieces]
    moves = [
        (j, targets.index(region[0]), *region[1:], offset)
        for j, (regions, offset, _) in enumerate(pieces)
        for region in regions
    ]
    kept = [outs[target] for target in targets if target in outs]
    placed = pl.pallas_call(
        functools.partial(place_body, count, moves, 0, len(arrays) + len(kept)),
        in_specs=[in_vmem] * len(arrays) + [in_hbm] * len(kept),
        out_specs=[in_hbm] * len(targets),
        out_shape=[jax.ShapeDtypeStruct(shapes[target], jnp.bfloat16) for target in targets],
        scratch_shapes=[pltpu.SemaphoreType.DMA((len(moves),))],
        input_output_aliases={len(arrays) + j: j for j in range(len(kept))},
        compiler_params=pltpu.CompilerParams(vmem_limit_bytes=4 << 20),
    )(*arrays, *kept)
    outs.update(zip(targets, placed))


def hops(count):
    plan = []
    for k in range(1, count):
        for name, source, parity in (("a", "b", 0), ("b", "a", 1)):
            pairs = []
            for i in range(parity, count - 1, 2):
                if i + k < count:
                    pairs.append((i + 1, i))
                if i + 1 - k >= 0:
                    pairs.append((i, i + 1))
            if pairs:
                offset = k if parity == 0 else -k
                plan.append((f"{name}{k}", f"{source}{k - 1}", pairs, offset))
    return plan


head = lanes
chunk_names = ("head", "body", "key", "value")


def groups(count):
    whole = (chunk_names,)
    return [whole] * (count - 2) + [(chunk_names[:-2], chunk_names[-2:-1], chunk_names[-1:])]


def by_line(count, cores, query, key, value, mixed, norms):
    rows, columns = query[0].shape[0], mixed[0].shape[1]
    used = norms[0].size // lanes
    packed = tiles(cores * used)
    pieces = {}
    pieces["head"] = merged_head(*mixed, head)
    pieces["body"], row = merged_body(mixed, query, norms, head)
    rows_of_cores = lax.all_gather(row, "width", axis=0, tiled=True)
    pieces["key"], pieces["value"] = merged_tail(key, value, rows_of_cores, cores, used)
    rest, halves = columns - head, mixed[0].shape[0] // rows
    wide = {name: weight[0].shape[1] for name, weight in (("query", query), ("key", key), ("value", value))}
    regions = {
        "head": [("mixed", 0, head, columns, 0, 0, 0)],
        "body": [("mixed", h * rest, rest, columns, head, 0, h * rows) for h in range(halves)]
        + [("query", halves * rest, wide["query"], 0, 0, rows, 0)],
        "key": [("key", b * wide["key"], wide["key"], 0, 0, rows, b * lanes) for b in range(rows // lanes)]
        + [("norm", wide["key"] * (rows // lanes), packed, packed, 0, 0, 0)],
        "value": [("value", 0, wide["value"], 0, 0, rows, 0)],
    }
    shapes = {name: (size, count * rows) for name, size in wide.items()}
    shapes["mixed"] = (count * columns, mixed[0].shape[0])
    shapes["norm"] = (count * packed, lanes)
    plan = hops(count)
    outs = {}
    held = {name: {"a0": piece, "b0": piece} for name, piece in pieces.items()}
    arrived = {name: [(regions[name], 0, piece)] for name, piece in pieces.items()}
    for k, parts in enumerate(groups(count), start=1):
        for hop, source, pairs, offset in plan:
            if int(hop[1:]) == k:
                for name in chunk_names:
                    held[name][hop] = lax.ppermute(held[name][source], "shard", pairs)
                    arrived[name].append((regions[name], offset, held[name][hop]))
        for part in parts:
            place(outs, shapes, [piece for name in part for piece in arrived[name]], count)
        arrived = {name: [] for name in chunk_names}
    serve_norm = outs["norm"].reshape(count, packed, lanes)[:, : cores * used].reshape(-1)
    return outs["query"], outs["key"], outs["value"], outs["mixed"], serve_norm


def by_gather(count, cores, query, key, value, mixed, norms):
    finals = []
    for axis, (w, low, high) in ((0, query), (0, key), (0, value), (1, mixed)):
        result = w.astype(jnp.float32) + mix_rate * jnp.dot(
            low, high, preferred_element_type=jnp.float32
        )
        narrow = result.astype(jnp.bfloat16)
        finals.append(lax.all_gather(narrow, "shard", axis=axis, tiled=True).T)
    norm = (norms[0] + norms[1]).astype(jnp.bfloat16)
    serve_norm = lax.all_gather(norm, ("shard", "width"), axis=0, tiled=True)
    return *finals, serve_norm


def on_device(form, count, cores, *args):
    weights = [args[3 * j : 3 * j + 3] for j in range(4)]
    return form(count, cores, *weights, args[12:])


def solution(mesh):
    column_cut = (P(("shift", "shard"), "width"), P(("shift", "shard"), None), P("shift", "width"))
    row_cut = (P(("shift", "width"), "shard"), P(("shift", "width"), None), P("shift", "shard"))
    norm = P(("shift", "shard", "width"))
    count, cores = mesh.shape["shard"], mesh.shape["width"]

    def step(*args):
        rows = args[0].shape[0] // (mesh.shape["shift"] * count)
        columns = args[9].shape[1] // count
        narrow = [args[j].shape[1] // cores for j in (0, 3, 6)]
        gains = args[12].shape[0] // (mesh.shape["shift"] * count * cores)
        aligned = all(size % (2 * lanes) == 0 for size in (rows, columns, *narrow, gains))
        tall = args[9].shape[0] // (mesh.shape["shift"] * cores)
        line = count > 2 and aligned and tall % rows == 0
        program = jax.shard_map(
            functools.partial(on_device, by_line if line else by_gather, count, cores),
            mesh=mesh,
            in_specs=(*column_cut, *column_cut, *column_cut, *row_cut, norm, norm),
            out_specs=(
                P(("shift", "width"), None),
                P(("shift", "width"), None),
                P(("shift", "width"), None),
                P("shift", "width"),
                P("shift"),
            ),
            check_vma=False,
        )
        return program(*args)

    return step
```

```python
import functools

import jax
import jax.numpy as jnp
from jax import lax
from jax.experimental import pallas as pl
from jax.experimental.pallas import tpu as pltpu
from jax.sharding import PartitionSpec as P


mix_rate = 0.5
lanes = 128
sublanes = 8


in_vmem = pl.BlockSpec(memory_space=pltpu.VMEM)
in_hbm = pl.BlockSpec(memory_space=pltpu.HBM)


def blocks(total):
    size = 2 * lanes
    return [(base, min(size, total - base)) for base in range(0, total, size)]


def stacked(out_ref, offset, total):
    width = out_ref.shape[1]

    def store(base, result):
        for h in range(result.shape[1] // width):
            row = pl.ds(offset + h * total + base, result.shape[0])
            out_ref[row, :] = result[:, h * width : (h + 1) * width]

    return store


def merge_into(store, total, first, w_ref, low_ref, high_ref, w_held, low_held, high_held, sems):
    copies = [
        pltpu.make_async_copy(low_ref, low_held, sems.at[0]),
        pltpu.make_async_copy(high_ref.at[:, pl.ds(first, total)], high_held, sems.at[1]),
    ]
    for j, (base, size) in enumerate(blocks(total)):
        source, target = w_ref.at[:, pl.ds(first + base, size)], w_held.at[:, pl.ds(base, size)]
        copies.append(pltpu.make_async_copy(source, target, sems.at[2 + j]))
    for copy in copies:
        copy.start()

    def finish():
        copies[0].wait()
        copies[1].wait()
        for (base, size), copy in zip(blocks(total), copies[2:]):
            copy.wait()
            part = pl.ds(base, size)
            delta = lax.dot_general(
                high_held[:, part],
                low_held[...],
                (((0,), (0,)), ((), ())),
                preferred_element_type=jnp.float32,
            )
            kept = w_held[:, part].T.astype(jnp.float32)
            store(base, (kept + mix_rate * delta).astype(jnp.bfloat16))

    return finish


def scratch_of(w, low, total):
    rows, rank = w.shape[0], low.shape[1]
    return [
        pltpu.VMEM((rows, total), jnp.bfloat16),
        pltpu.VMEM((rank, rows), jnp.bfloat16),
        pltpu.VMEM((rank, total), jnp.bfloat16),
        pltpu.SemaphoreType.DMA((2 + len(blocks(total)),)),
    ]


def hbm(*arrays):
    return [pltpu.with_memory_space_constraint(a, pltpu.HBM) for a in arrays]


def tiles(rows):
    return -(-rows // sublanes) * sublanes


merge_params = pltpu.CompilerParams(vmem_limit_bytes=12 << 20)


def merged_head(w, low, high, head):
    ahead = pl.ds(0, head)

    def body(w_ref, low_ref, high_ref, out_ref, w_held, low_held, high_held, sems):
        copies = [
            pltpu.make_async_copy(w_ref.at[:, ahead], w_held, sems.at[0]),
            pltpu.make_async_copy(low_ref, low_held, sems.at[1]),
            pltpu.make_async_copy(high_ref.at[:, ahead], high_held, sems.at[2]),
        ]
        for copy in copies:
            copy.start()
        copies[1].wait()
        copies[2].wait()
        delta = lax.dot_general(
            high_held[...],
            low_held[...],
            (((0,), (0,)), ((), ())),
            preferred_element_type=jnp.float32,
        )
        copies[0].wait()
        kept = w_held[...].T.astype(jnp.float32)
        out_ref[...] = (kept + mix_rate * delta).astype(jnp.bfloat16)

    return pl.pallas_call(
        body,
        in_specs=[in_hbm] * 3,
        out_specs=in_vmem,
        out_shape=jax.ShapeDtypeStruct((head, w.shape[0]), jnp.bfloat16),
        scratch_shapes=scratch_of(w, low, head),
        compiler_params=merge_params,
    )(*hbm(w, low.T, high))


def merged_body(mixed, query, norms, head):
    rest, width, wide = mixed[0].shape[1] - head, query[0].shape[0], query[0].shape[1]
    below = rest * (mixed[0].shape[0] // width)
    used = norms[0].size // lanes
    tall = tiles(used)
    held = 4

    def body(wm, lm, hm, wq, lq, hq, train, step, out_ref, row_ref, *scratch):
        keep = stacked(out_ref, below, wide)
        share = stacked(row_ref, tall, shared)

        def store(base, result):
            last = base + result.shape[0] == wide
            kept = result.shape[0] - (shared if last else 0)
            keep(base, result[:kept])
            if last:
                share(0, result[kept:])

        finish_mixed = merge_into(stacked(out_ref, 0, rest), rest, head, wm, lm, hm, *scratch[:held])
        finish_query = merge_into(store, wide, 0, wq, lq, hq, *scratch[held : 2 * held])
        train_held, step_held, sems = scratch[2 * held :]
        copies = [
            pltpu.make_async_copy(train, train_held, sems.at[0]),
            pltpu.make_async_copy(step, step_held, sems.at[1]),
        ]
        for copy in copies:
            copy.start()
        finish_mixed()
        finish_query()
        for copy in copies:
            copy.wait()
        row_ref[:tall, :] = jnp.zeros((tall, lanes), jnp.bfloat16)
        row_ref[:used, :] = (train_held[...] + step_held[...]).astype(jnp.bfloat16)

    return pl.pallas_call(
        body,
        in_specs=[in_hbm] * 8,
        out_specs=[in_vmem] * 2,
        out_shape=[
            jax.ShapeDtypeStruct((below + wide - shared, width), jnp.bfloat16),
            jax.ShapeDtypeStruct((tall + shared * (width // lanes), lanes), jnp.bfloat16),
        ],
        scratch_shapes=[
            *scratch_of(mixed[0], mixed[1], rest),
            *scratch_of(query[0], query[1], wide),
            *[pltpu.VMEM((used, lanes), jnp.float32)] * 2,
            pltpu.SemaphoreType.DMA((2,)),
        ],
        compiler_params=merge_params,
    )(
        *hbm(mixed[0], mixed[1].T, mixed[2], query[0], query[1].T, query[2]),
        *hbm(*(a.reshape(used, lanes) for a in norms)),
    )


def merged_tail(*weights):
    held = 4

    def body(*refs):
        outs, scratch = refs[3 * len(weights) :][: len(weights)], refs[4 * len(weights) :]
        finishes = [
            merge_into(
                stacked(outs[j], 0, outs[j].shape[0]),
                outs[j].shape[0],
                0,
                *refs[3 * j : 3 * j + 3],
                *scratch[held * j : held * (j + 1)],
            )
            for j in range(len(weights))
        ]
        for finish in finishes:
            finish()

    return pl.pallas_call(
        body,
        in_specs=[in_hbm] * (3 * len(weights)),
        out_specs=[in_vmem] * len(weights),
        out_shape=[jax.ShapeDtypeStruct(w.shape[::-1], jnp.bfloat16) for w, _, _ in weights],
        scratch_shapes=[ref for w, low, _ in weights for ref in scratch_of(w, low, w.shape[1])],
        compiler_params=merge_params,
    )(*hbm(*(a for w, low, high in weights for a in (w, low.T, high))))


def place_shared(query_out, gathered, count, cores, tall, extent):
    stacks = extent // lanes
    each = tall + shared * stacks
    low = query_out.shape[0] - shared

    def body(gathered_ref, _, out_ref, sems):
        mine = lax.axis_index("width") * each + tall
        for act in ("start", "wait"):
            for owner in range(count):
                for b in range(stacks):
                    at = ((cores - 1) * count + owner) * cores * each + b * shared
                    source = gathered_ref.at[pl.ds(pl.multiple_of(mine + at, sublanes), shared)]
                    target = out_ref.at[pl.ds(low, shared), pl.ds(owner * extent + b * lanes, lanes)]
                    getattr(pltpu.make_async_copy(source, target, sems.at[owner * stacks + b]), act)()

    return pl.pallas_call(
        body,
        in_specs=[in_vmem, in_hbm],
        out_specs=in_hbm,
        out_shape=jax.ShapeDtypeStruct(query_out.shape, query_out.dtype),
        scratch_shapes=[pltpu.SemaphoreType.DMA((count * stacks,))],
        input_output_aliases={1: 0},
        compiler_params=pltpu.CompilerParams(vmem_limit_bytes=4 << 20),
    )(gathered, query_out)


def place_body(count, moves, pieces_at, outs_at, *refs):
    sems = refs[-1]
    me = lax.axis_index("shard")
    sign = 1 - 2 * lax.rem(me, 2)
    for act in ("start", "wait"):
        for j, (piece, out, low, rows, tall, down, wide, right, offset) in enumerate(moves):
            owner = me + sign * offset

            @pl.when(jnp.logical_and(owner >= 0, owner < count))
            def _():
                source = refs[pieces_at + piece].at[pl.ds(low, rows)]
                row = pl.multiple_of(owner * tall + down, sublanes)
                column = pl.multiple_of(owner * wide + right, lanes)
                target = refs[outs_at + out].at[pl.ds(row, rows), pl.ds(column, source.shape[1])]
                getattr(pltpu.make_async_copy(source, target, sems.at[j]), act)()


def place(outs, shapes, pieces, count):
    targets = list(dict.fromkeys(region[0] for regions, _, _ in pieces for region in regions))
    arrays = [array for _, _, array in pieces]
    moves = [
        (j, targets.index(region[0]), *region[1:], offset)
        for j, (regions, offset, _) in enumerate(pieces)
        for region in regions
    ]
    kept = [outs[target] for target in targets if target in outs]
    placed = pl.pallas_call(
        functools.partial(place_body, count, moves, 0, len(arrays) + len(kept)),
        in_specs=[in_vmem] * len(arrays) + [in_hbm] * len(kept),
        out_specs=[in_hbm] * len(targets),
        out_shape=[jax.ShapeDtypeStruct(shapes[target], jnp.bfloat16) for target in targets],
        scratch_shapes=[pltpu.SemaphoreType.DMA((len(moves),))],
        input_output_aliases={len(arrays) + j: j for j in range(len(kept))},
        compiler_params=pltpu.CompilerParams(vmem_limit_bytes=4 << 20),
    )(*arrays, *kept)
    outs.update(zip(targets, placed))


def hops(count):
    plan = []
    for k in range(1, count):
        for name, source, parity in (("a", "b", 0), ("b", "a", 1)):
            pairs = []
            for i in range(parity, count - 1, 2):
                if i + k < count:
                    pairs.append((i + 1, i))
                if i + 1 - k >= 0:
                    pairs.append((i, i + 1))
            if pairs:
                offset = k if parity == 0 else -k
                plan.append((f"{name}{k}", f"{source}{k - 1}", pairs, offset))
    return plan


head = lanes
shared = 2 * sublanes
chunk_names = ("head", "body", "shared", "key", "value")


def groups(count):
    whole = (chunk_names,)
    return [whole] * (count - 2) + [(chunk_names[:-2], chunk_names[-2:-1], chunk_names[-1:])]


def by_line(count, cores, query, key, value, mixed, norms):
    rows, columns = query[0].shape[0], mixed[0].shape[1]
    used = norms[0].size // lanes
    tall = tiles(used)
    pieces = {}
    pieces["head"] = merged_head(*mixed, head)
    pieces["body"], row = merged_body(mixed, query, norms, head)
    pieces["shared"] = lax.all_gather(row, "width", axis=0, tiled=True)
    pieces["key"], pieces["value"] = merged_tail(key, value)
    rest, halves = columns - head, mixed[0].shape[0] // rows
    wide = {name: weight[0].shape[1] for name, weight in (("query", query), ("key", key), ("value", value))}
    both = pieces["shared"].shape[0]
    regions = {
        "head": [("mixed", 0, head, columns, 0, 0, 0)],
        "body": [("mixed", h * rest, rest, columns, head, 0, h * rows) for h in range(halves)]
        + [("query", halves * rest, wide["query"] - shared, 0, 0, rows, 0)],
        "shared": [("shared", 0, both, both, 0, 0, 0)],
        "key": [("key", 0, wide["key"], 0, 0, rows, 0)],
        "value": [("value", 0, wide["value"], 0, 0, rows, 0)],
    }
    shapes = {name: (size, count * rows) for name, size in wide.items()}
    shapes["mixed"] = (count * columns, mixed[0].shape[0])
    shapes["shared"] = (count * both, lanes)
    plan = hops(count)
    outs = {}
    held = {name: {"a0": piece, "b0": piece} for name, piece in pieces.items()}
    arrived = {name: [(regions[name], 0, piece)] for name, piece in pieces.items()}
    for k, parts in enumerate(groups(count), start=1):
        for hop, source, pairs, offset in plan:
            if int(hop[1:]) == k:
                for name in chunk_names:
                    if name == "shared":
                        last = [(i * cores + cores - 1, j * cores + cores - 1) for i, j in pairs]
                        held[name][hop] = lax.ppermute(held[name][source], ("shard", "width"), last)
                    else:
                        held[name][hop] = lax.ppermute(held[name][source], "shard", pairs)
                    arrived[name].append((regions[name], offset, held[name][hop]))
        for part in parts:
            place(outs, shapes, [piece for name in part for piece in arrived[name]], count)
        arrived = {name: [] for name in chunk_names}
    gathered = lax.all_gather(outs["shared"], "width", axis=0, tiled=True)
    final_query = place_shared(outs["query"], gathered, count, cores, tall, rows)
    sums = gathered[(cores - 1) * count * both :].reshape(count * cores, both // cores, lanes)
    serve_norm = sums[:, :used].reshape(-1)
    return final_query, outs["key"], outs["value"], outs["mixed"], serve_norm


def by_gather(count, cores, query, key, value, mixed, norms):
    finals = []
    for axis, (w, low, high) in ((0, query), (0, key), (0, value), (1, mixed)):
        result = w.astype(jnp.float32) + mix_rate * jnp.dot(
            low, high, preferred_element_type=jnp.float32
        )
        narrow = result.astype(jnp.bfloat16)
        finals.append(lax.all_gather(narrow, "shard", axis=axis, tiled=True).T)
    norm = (norms[0] + norms[1]).astype(jnp.bfloat16)
    serve_norm = lax.all_gather(norm, ("shard", "width"), axis=0, tiled=True)
    return *finals, serve_norm


def on_device(form, count, cores, *args):
    weights = [args[3 * j : 3 * j + 3] for j in range(4)]
    return form(count, cores, *weights, args[12:])


def solution(mesh):
    column_cut = (P(("shift", "shard"), "width"), P(("shift", "shard"), None), P("shift", "width"))
    row_cut = (P(("shift", "width"), "shard"), P(("shift", "width"), None), P("shift", "shard"))
    norm = P(("shift", "shard", "width"))
    count, cores = mesh.shape["shard"], mesh.shape["width"]

    def step(*args):
        rows = args[0].shape[0] // (mesh.shape["shift"] * count)
        columns = args[9].shape[1] // count
        narrow = [args[j].shape[1] // cores for j in (0, 3, 6)]
        gains = args[12].shape[0] // (mesh.shape["shift"] * count * cores)
        aligned = all(size % (2 * lanes) == 0 for size in (rows, columns, *narrow, gains))
        tall = args[9].shape[0] // (mesh.shape["shift"] * cores)
        line = count > 2 and aligned and tall % rows == 0
        program = jax.shard_map(
            functools.partial(on_device, by_line if line else by_gather, count, cores),
            mesh=mesh,
            in_specs=(*column_cut, *column_cut, *column_cut, *row_cut, norm, norm),
            out_specs=(
                P(("shift", "width"), None),
                P(("shift", "width"), None),
                P(("shift", "width"), None),
                P("shift", "width"),
                P("shift"),
            ),
            check_vma=False,
        )
        return program(*args)

    return step
```

```python
import functools

import jax
import jax.numpy as jnp
from jax import lax
from jax.experimental import pallas as pl
from jax.experimental.pallas import tpu as pltpu
from jax.sharding import PartitionSpec as P


mix_rate = 0.5
lanes = 128
sublanes = 8


in_vmem = pl.BlockSpec(memory_space=pltpu.VMEM)
in_hbm = pl.BlockSpec(memory_space=pltpu.HBM)


def blocks(total):
    size = 2 * lanes
    return [(base, min(size, total - base)) for base in range(0, total, size)]


def merge_into(out_ref, offset, total, first, w_ref, low_ref, high_ref, w_held, low_held, high_held, sems):
    copies = [
        pltpu.make_async_copy(low_ref, low_held, sems.at[0]),
        pltpu.make_async_copy(high_ref.at[:, pl.ds(first, total)], high_held, sems.at[1]),
    ]
    for j, (base, size) in enumerate(blocks(total)):
        source, target = w_ref.at[:, pl.ds(first + base, size)], w_held.at[:, pl.ds(base, size)]
        copies.append(pltpu.make_async_copy(source, target, sems.at[2 + j]))
    for copy in copies:
        copy.start()

    def finish():
        copies[0].wait()
        copies[1].wait()
        width = out_ref.shape[1]
        for (base, size), copy in zip(blocks(total), copies[2:]):
            copy.wait()
            part = pl.ds(base, size)
            delta = lax.dot_general(
                high_held[:, part],
                low_held[...],
                (((0,), (0,)), ((), ())),
                preferred_element_type=jnp.float32,
            )
            kept = w_held[:, part].T.astype(jnp.float32)
            result = (kept + mix_rate * delta).astype(jnp.bfloat16)
            for h in range(w_held.shape[0] // width):
                row = offset + h * total + base
                out_ref[pl.ds(row, size), :] = result[:, h * width : (h + 1) * width]

    return finish


def scratch_of(w, low, total):
    rows, rank = w.shape[0], low.shape[1]
    return [
        pltpu.VMEM((rows, total), jnp.bfloat16),
        pltpu.VMEM((rank, rows), jnp.bfloat16),
        pltpu.VMEM((rank, total), jnp.bfloat16),
        pltpu.SemaphoreType.DMA((2 + len(blocks(total)),)),
    ]


def hbm(*arrays):
    return [pltpu.with_memory_space_constraint(a, pltpu.HBM) for a in arrays]


def tiles(rows):
    return -(-rows // sublanes) * sublanes


merge_params = pltpu.CompilerParams(vmem_limit_bytes=12 << 20)


def merged(weights, extra=()):
    held, count = 4, len(weights)
    shapes = [
        jax.ShapeDtypeStruct((w.shape[1] * (w.shape[0] // width), width), jnp.bfloat16)
        for w, _, _, width in weights
    ]
    scratch_shapes = [ref for w, low, _, _ in weights for ref in scratch_of(w, low, w.shape[1])]
    operands = hbm(*(a for w, low, high, _ in weights for a in (w, low.T, high)))
    if extra:
        part, rank, used = extra[3], extra[0].shape[1], extra[1].size // lanes
        blocks_of_low = part // lanes
        operands += hbm(extra[0].T, *(a.reshape(used, lanes) for a in extra[1:3]))
        side = rank * blocks_of_low
        shapes.append(jax.ShapeDtypeStruct((side + tiles(used), lanes), jnp.bfloat16))
        scratch_shapes += [pltpu.VMEM((rank, part), jnp.bfloat16)]
        scratch_shapes += [pltpu.VMEM((used, lanes), jnp.float32)] * 2
        scratch_shapes += [pltpu.SemaphoreType.DMA((3,))]

    def body(*refs):
        inputs, outs = refs[: len(operands)], refs[len(operands) :][: len(shapes)]
        scratch = refs[len(operands) + len(shapes) :]
        finishes = [
            merge_into(
                outs[j], 0, inputs[3 * j].shape[1], 0, *inputs[3 * j : 3 * j + 3], *scratch[held * j : held * j + held]
            )
            for j in range(count)
        ]
        if extra:
            targets, sems = scratch[held * count : -1], scratch[-1]
            low_ref, train, step = inputs[3 * count :]
            mine = pl.ds(pl.multiple_of(lax.axis_index("width") * part, lanes), part)
            copies = [
                pltpu.make_async_copy(source, target, sems.at[j])
                for j, (source, target) in enumerate(zip((low_ref.at[:, mine], train, step), targets))
            ]
            for copy in copies:
                copy.start()
        for finish in finishes:
            finish()
        if extra:
            for copy in copies:
                copy.wait()
            low_held, train_held, step_held = targets
            for j in range(blocks_of_low):
                outs[-1][pl.ds(j * rank, rank), :] = low_held[:, pl.ds(j * lanes, lanes)]
            outs[-1][pl.ds(side, tiles(used)), :] = jnp.zeros((tiles(used), lanes), jnp.bfloat16)
            outs[-1][pl.ds(side, used), :] = (train_held[...] + step_held[...]).astype(jnp.bfloat16)

    return pl.pallas_call(
        body,
        in_specs=[in_hbm] * len(operands),
        out_specs=[in_vmem] * len(shapes),
        out_shape=shapes,
        scratch_shapes=scratch_shapes,
        compiler_params=merge_params,
    )(*operands)


def merged_pieces(pieces, sides, high, count, cores, each):
    rows, wide = pieces[0][1].shape
    rank = high.shape[0]
    stacks = rows // lanes // cores
    offsets = [offset for offset, _ in pieces]
    total = len(pieces)

    def body(*refs):
        raws, sides_ref, high_ref, out_ref = refs[:total], refs[total], refs[total + 1], refs[total + 2]
        low_held, result, low_sems, out_sems = refs[total + 3 :]
        me = lax.axis_index("shard")
        sign = 1 - 2 * lax.rem(me, 2)
        for act in ("work", "wait"):
            for j, offset in enumerate(offsets):
                owner = me + sign * offset

                @pl.when(jnp.logical_and(owner >= 0, owner < count))
                def _():
                    column = pl.multiple_of(owner * rows, lanes)
                    move = pltpu.make_async_copy(
                        result.at[j], out_ref.at[:, pl.ds(column, rows)], out_sems.at[j]
                    )
                    if act == "wait":
                        move.wait()
                        return
                    copies = []
                    for core in range(cores):
                        for b in range(stacks):
                            at = pl.multiple_of((core * count + owner) * each + b * rank, sublanes)
                            n = core * stacks + b
                            copies.append(
                                pltpu.make_async_copy(
                                    sides_ref.at[pl.ds(at, rank)],
                                    low_held.at[j, :, pl.ds(n * lanes, lanes)],
                                    low_sems.at[n],
                                )
                            )
                    for copy in copies:
                        copy.start()
                    for copy in copies:
                        copy.wait()
                    delta = lax.dot_general(
                        high_ref[...],
                        low_held[j],
                        (((0,), (0,)), ((), ())),
                        preferred_element_type=jnp.float32,
                    )
                    kept = raws[j][...].T.astype(jnp.float32)
                    result[j] = (kept + mix_rate * delta).astype(jnp.bfloat16)
                    move.start()

    return pl.pallas_call(
        body,
        in_specs=[in_vmem] * (total + 2),
        out_specs=in_hbm,
        out_shape=jax.ShapeDtypeStruct((wide, count * rows), jnp.bfloat16),
        scratch_shapes=[
            pltpu.VMEM((total, rank, rows), jnp.bfloat16),
            pltpu.VMEM((total, wide, rows), jnp.bfloat16),
            pltpu.SemaphoreType.DMA((cores * stacks,)),
            pltpu.SemaphoreType.DMA((total,)),
        ],
        compiler_params=merge_params,
    )(*(w for _, w in pieces), sides, high)


def place_body(count, moves, pieces_at, outs_at, *refs):
    sems = refs[-1]
    me = lax.axis_index("shard")
    sign = 1 - 2 * lax.rem(me, 2)
    for act in ("start", "wait"):
        for j, (piece, out, low, rows, tall, down, wide, right, offset) in enumerate(moves):
            owner = me + sign * offset

            @pl.when(jnp.logical_and(owner >= 0, owner < count))
            def _():
                source = refs[pieces_at + piece].at[pl.ds(low, rows)]
                row = pl.multiple_of(owner * tall + down, sublanes)
                column = pl.multiple_of(owner * wide + right, lanes)
                target = refs[outs_at + out].at[pl.ds(row, rows), pl.ds(column, source.shape[1])]
                getattr(pltpu.make_async_copy(source, target, sems.at[j]), act)()


def place(outs, shapes, pieces, count):
    targets = list(dict.fromkeys(region[0] for regions, _, _ in pieces for region in regions))
    arrays = [array for _, _, array in pieces]
    moves = [
        (j, targets.index(region[0]), *region[1:], offset)
        for j, (regions, offset, _) in enumerate(pieces)
        for region in regions
    ]
    kept = [outs[target] for target in targets if target in outs]
    placed = pl.pallas_call(
        functools.partial(place_body, count, moves, 0, len(arrays) + len(kept)),
        in_specs=[in_vmem] * len(arrays) + [in_hbm] * len(kept),
        out_specs=[in_hbm] * len(targets),
        out_shape=[jax.ShapeDtypeStruct(shapes[target], jnp.bfloat16) for target in targets],
        scratch_shapes=[pltpu.SemaphoreType.DMA((len(moves),))],
        input_output_aliases={len(arrays) + j: j for j in range(len(kept))},
        compiler_params=pltpu.CompilerParams(vmem_limit_bytes=4 << 20),
    )(*arrays, *kept)
    outs.update(zip(targets, placed))


def hops(count):
    plan = []
    for k in range(1, count):
        for name, source, parity in (("a", "b", 0), ("b", "a", 1)):
            pairs = []
            for i in range(parity, count - 1, 2):
                if i + k < count:
                    pairs.append((i + 1, i))
                if i + 1 - k >= 0:
                    pairs.append((i, i + 1))
            if pairs:
                offset = k if parity == 0 else -k
                plan.append((f"{name}{k}", f"{source}{k - 1}", pairs, offset))
    return plan


chunk_names = ("key", "mixed", "side", "query", "value")
late = ("mixed", "side", "query", "value")


def groups(count):
    return [(late,)] * (count - 2) + [(late[:2], late[2:3], late[3:])]


def by_line(count, cores, query, key, value, mixed, norms):
    rows, columns = query[0].shape[0], mixed[0].shape[1]
    used = norms[0].size // lanes
    part = rows // cores
    pieces = {"key": key[0]}
    pieces["mixed"], pieces["side"] = merged([(*mixed, rows)], (key[1], *norms, part))
    pieces["query"], pieces["value"] = merged([(*query, rows), (*value, rows)])
    each = pieces["side"].shape[0]
    wide = {name: weight[0].shape[1] for name, weight in (("query", query), ("value", value))}
    regions = {
        "mixed": [
            ("mixed", h * columns, columns, columns, 0, 0, h * rows)
            for h in range(mixed[0].shape[0] // rows)
        ],
        "side": [("side", 0, each, each, 0, 0, 0)],
        "query": [("query", 0, wide["query"], 0, 0, rows, 0)],
        "value": [("value", 0, wide["value"], 0, 0, rows, 0)],
    }
    shapes = {name: (size, count * rows) for name, size in wide.items()}
    shapes["mixed"] = (count * columns, mixed[0].shape[0])
    shapes["side"] = (count * each, lanes)
    plan = hops(count)
    outs = {}
    held = {name: {"a0": piece, "b0": piece} for name, piece in pieces.items()}
    raw = [(0, key[0])]
    arrived = {name: [(regions[name], 0, pieces[name])] for name in late}
    for k, parts in enumerate(groups(count), start=1):
        for hop, source, pairs, offset in plan:
            if int(hop[1:]) == k:
                for name in chunk_names:
                    held[name][hop] = lax.ppermute(held[name][source], "shard", pairs)
                    if name in late:
                        arrived[name].append((regions[name], offset, held[name][hop]))
                raw.append((offset, held["key"][hop]))
        for part in parts:
            place(outs, shapes, [piece for name in part for piece in arrived[name]], count)
        arrived = {name: [] for name in late}
    sides = lax.all_gather(outs["side"], "width", axis=0, tiled=True)
    final_key = merged_pieces(raw, sides, key[2], count, cores, each)
    sums = sides.reshape(cores, count, each, lanes)[:, :, each - tiles(used) :][:, :, :used]
    serve_norm = sums.transpose(1, 0, 2, 3).reshape(-1)
    return outs["query"], final_key, outs["value"], outs["mixed"], serve_norm


def by_gather(count, cores, query, key, value, mixed, norms):
    finals = []
    for axis, (w, low, high) in ((0, query), (0, key), (0, value), (1, mixed)):
        result = w.astype(jnp.float32) + mix_rate * jnp.dot(
            low, high, preferred_element_type=jnp.float32
        )
        narrow = result.astype(jnp.bfloat16)
        finals.append(lax.all_gather(narrow, "shard", axis=axis, tiled=True).T)
    norm = (norms[0] + norms[1]).astype(jnp.bfloat16)
    serve_norm = lax.all_gather(norm, ("shard", "width"), axis=0, tiled=True)
    return *finals, serve_norm


def on_device(form, count, cores, *args):
    weights = [args[3 * j : 3 * j + 3] for j in range(4)]
    return form(count, cores, *weights, args[12:])


def solution(mesh):
    column_cut = (P(("shift", "shard"), "width"), P(("shift", "shard"), None), P("shift", "width"))
    row_cut = (P(("shift", "width"), "shard"), P(("shift", "width"), None), P("shift", "shard"))
    norm = P(("shift", "shard", "width"))
    count, cores = mesh.shape["shard"], mesh.shape["width"]

    def step(*args):
        rows = args[0].shape[0] // (mesh.shape["shift"] * count)
        columns = args[9].shape[1] // count
        narrow = [args[j].shape[1] // cores for j in (0, 3, 6)]
        gains = args[12].shape[0] // (mesh.shape["shift"] * count * cores)
        aligned = all(size % (2 * lanes) == 0 for size in (rows, columns, *narrow, gains))
        tall = args[9].shape[0] // (mesh.shape["shift"] * cores)
        line = count > 2 and aligned and tall % rows == 0 and rows % (cores * lanes) == 0
        program = jax.shard_map(
            functools.partial(on_device, by_line if line else by_gather, count, cores),
            mesh=mesh,
            in_specs=(*column_cut, *column_cut, *column_cut, *row_cut, norm, norm),
            out_specs=(
                P(("shift", "width"), None),
                P(("shift", "width"), None),
                P(("shift", "width"), None),
                P("shift", "width"),
                P("shift"),
            ),
            check_vma=False,
        )
        return program(*args)

    return step
```

```python
import functools

import jax
import jax.numpy as jnp
from jax import lax
from jax.experimental import pallas as pl
from jax.experimental.pallas import tpu as pltpu
from jax.sharding import PartitionSpec as P


mix_rate = 0.5
lanes = 128
sublanes = 8


in_vmem = pl.BlockSpec(memory_space=pltpu.VMEM)
in_hbm = pl.BlockSpec(memory_space=pltpu.HBM)


def blocks(total):
    size = 2 * lanes
    return [(base, min(size, total - base)) for base in range(0, total, size)]


def merge_into(out_ref, offset, total, first, w_ref, low_ref, high_ref, w_held, low_held, high_held, sems):
    copies = [
        pltpu.make_async_copy(low_ref, low_held, sems.at[0]),
        pltpu.make_async_copy(high_ref.at[:, pl.ds(first, total)], high_held, sems.at[1]),
    ]
    for j, (base, size) in enumerate(blocks(total)):
        source, target = w_ref.at[:, pl.ds(first + base, size)], w_held.at[:, pl.ds(base, size)]
        copies.append(pltpu.make_async_copy(source, target, sems.at[2 + j]))
    for copy in copies:
        copy.start()

    def finish():
        copies[0].wait()
        copies[1].wait()
        width = out_ref.shape[1]
        for (base, size), copy in zip(blocks(total), copies[2:]):
            copy.wait()
            part = pl.ds(base, size)
            delta = lax.dot_general(
                high_held[:, part],
                low_held[...],
                (((0,), (0,)), ((), ())),
                preferred_element_type=jnp.float32,
            )
            kept = w_held[:, part].T.astype(jnp.float32)
            result = (kept + mix_rate * delta).astype(jnp.bfloat16)
            for h in range(w_held.shape[0] // width):
                row = offset + h * total + base
                out_ref[pl.ds(row, size), :] = result[:, h * width : (h + 1) * width]

    return finish


def scratch_of(w, low, total):
    rows, rank = w.shape[0], low.shape[1]
    return [
        pltpu.VMEM((rows, total), jnp.bfloat16),
        pltpu.VMEM((rank, rows), jnp.bfloat16),
        pltpu.VMEM((rank, total), jnp.bfloat16),
        pltpu.SemaphoreType.DMA((2 + len(blocks(total)),)),
    ]


def hbm(*arrays):
    return [pltpu.with_memory_space_constraint(a, pltpu.HBM) for a in arrays]


def tiles(rows):
    return -(-rows // sublanes) * sublanes


merge_params = pltpu.CompilerParams(vmem_limit_bytes=12 << 20)


def merged(weights, extra=()):
    held, count = 4, len(weights)
    shapes = [
        jax.ShapeDtypeStruct((w.shape[1] * (w.shape[0] // width), width), jnp.bfloat16)
        for w, _, _, width in weights
    ]
    scratch_shapes = [ref for w, low, _, _ in weights for ref in scratch_of(w, low, w.shape[1])]
    operands = hbm(*(a for w, low, high, _ in weights for a in (w, low.T, high)))
    if extra:
        part, rank, used = extra[3], extra[0].shape[1], extra[1].size // lanes
        blocks_of_low = part // lanes
        operands += hbm(extra[0].T, *(a.reshape(used, lanes) for a in extra[1:3]))
        under = shapes[0].shape[0]
        side = under + rank * blocks_of_low
        shapes[0] = jax.ShapeDtypeStruct((side + tiles(used), lanes), jnp.bfloat16)
        scratch_shapes += [pltpu.VMEM((rank, part), jnp.bfloat16)]
        scratch_shapes += [pltpu.VMEM((used, lanes), jnp.float32)] * 2
        scratch_shapes += [pltpu.SemaphoreType.DMA((3,))]

    def body(*refs):
        inputs, outs = refs[: len(operands)], refs[len(operands) :][: len(shapes)]
        scratch = refs[len(operands) + len(shapes) :]
        finishes = [
            merge_into(
                outs[j], 0, inputs[3 * j].shape[1], 0, *inputs[3 * j : 3 * j + 3], *scratch[held * j : held * j + held]
            )
            for j in range(count)
        ]
        if extra:
            targets, sems = scratch[held * count : -1], scratch[-1]
            low_ref, train, step = inputs[3 * count :]
            mine = pl.ds(pl.multiple_of(lax.axis_index("width") * part, lanes), part)
            copies = [
                pltpu.make_async_copy(source, target, sems.at[j])
                for j, (source, target) in enumerate(zip((low_ref.at[:, mine], train, step), targets))
            ]
            for copy in copies:
                copy.start()
        for finish in finishes:
            finish()
        if extra:
            for copy in copies:
                copy.wait()
            low_held, train_held, step_held = targets
            for j in range(blocks_of_low):
                outs[0][pl.ds(under + j * rank, rank), :] = low_held[:, pl.ds(j * lanes, lanes)]
            outs[0][pl.ds(side, tiles(used)), :] = jnp.zeros((tiles(used), lanes), jnp.bfloat16)
            outs[0][pl.ds(side, used), :] = (train_held[...] + step_held[...]).astype(jnp.bfloat16)

    return pl.pallas_call(
        body,
        in_specs=[in_hbm] * len(operands),
        out_specs=[in_vmem] * len(shapes),
        out_shape=shapes,
        scratch_shapes=scratch_shapes,
        compiler_params=merge_params,
    )(*operands)


def merged_pieces(pieces, sides, high, count, cores, each):
    rows, wide = pieces[0][1].shape
    rank = high.shape[0]
    stacks = rows // lanes // cores
    offsets = [offset for offset, _ in pieces]
    total = len(pieces)

    def body(*refs):
        raws, sides_ref, high_ref, out_ref = refs[:total], refs[total], refs[total + 1], refs[total + 2]
        low_held, result, low_sems, out_sems = refs[total + 3 :]
        me = lax.axis_index("shard")
        sign = 1 - 2 * lax.rem(me, 2)
        for act in ("work", "wait"):
            for j, offset in enumerate(offsets):
                owner = me + sign * offset

                @pl.when(jnp.logical_and(owner >= 0, owner < count))
                def _():
                    column = pl.multiple_of(owner * rows, lanes)
                    move = pltpu.make_async_copy(
                        result.at[j], out_ref.at[:, pl.ds(column, rows)], out_sems.at[j]
                    )
                    if act == "wait":
                        move.wait()
                        return
                    copies = []
                    for core in range(cores):
                        for b in range(stacks):
                            at = pl.multiple_of((core * count + owner) * each + b * rank, sublanes)
                            n = core * stacks + b
                            copies.append(
                                pltpu.make_async_copy(
                                    sides_ref.at[pl.ds(at, rank)],
                                    low_held.at[j, :, pl.ds(n * lanes, lanes)],
                                    low_sems.at[n],
                                )
                            )
                    for copy in copies:
                        copy.start()
                    for copy in copies:
                        copy.wait()
                    delta = lax.dot_general(
                        high_ref[...],
                        low_held[j],
                        (((0,), (0,)), ((), ())),
                        preferred_element_type=jnp.float32,
                    )
                    kept = raws[j][...].T.astype(jnp.float32)
                    result[j] = (kept + mix_rate * delta).astype(jnp.bfloat16)
                    move.start()

    return pl.pallas_call(
        body,
        in_specs=[in_vmem] * (total + 2),
        out_specs=in_hbm,
        out_shape=jax.ShapeDtypeStruct((wide, count * rows), jnp.bfloat16),
        scratch_shapes=[
            pltpu.VMEM((total, rank, rows), jnp.bfloat16),
            pltpu.VMEM((total, wide, rows), jnp.bfloat16),
            pltpu.SemaphoreType.DMA((cores * stacks,)),
            pltpu.SemaphoreType.DMA((total,)),
        ],
        compiler_params=merge_params,
    )(*(w for _, w in pieces), sides, high)


def place_body(count, moves, pieces_at, outs_at, *refs):
    sems = refs[-1]
    me = lax.axis_index("shard")
    sign = 1 - 2 * lax.rem(me, 2)
    for act in ("start", "wait"):
        for j, (piece, out, low, rows, tall, down, wide, right, offset) in enumerate(moves):
            owner = me + sign * offset

            @pl.when(jnp.logical_and(owner >= 0, owner < count))
            def _():
                source = refs[pieces_at + piece].at[pl.ds(low, rows)]
                row = pl.multiple_of(owner * tall + down, sublanes)
                column = pl.multiple_of(owner * wide + right, lanes)
                target = refs[outs_at + out].at[pl.ds(row, rows), pl.ds(column, source.shape[1])]
                getattr(pltpu.make_async_copy(source, target, sems.at[j]), act)()


def place(outs, shapes, pieces, count):
    targets = list(dict.fromkeys(region[0] for regions, _, _ in pieces for region in regions))
    arrays = [array for _, _, array in pieces]
    moves = [
        (j, targets.index(region[0]), *region[1:], offset)
        for j, (regions, offset, _) in enumerate(pieces)
        for region in regions
    ]
    kept = [outs[target] for target in targets if target in outs]
    placed = pl.pallas_call(
        functools.partial(place_body, count, moves, 0, len(arrays) + len(kept)),
        in_specs=[in_vmem] * len(arrays) + [in_hbm] * len(kept),
        out_specs=[in_hbm] * len(targets),
        out_shape=[jax.ShapeDtypeStruct(shapes[target], jnp.bfloat16) for target in targets],
        scratch_shapes=[pltpu.SemaphoreType.DMA((len(moves),))],
        input_output_aliases={len(arrays) + j: j for j in range(len(kept))},
        compiler_params=pltpu.CompilerParams(vmem_limit_bytes=4 << 20),
    )(*arrays, *kept)
    outs.update(zip(targets, placed))


def hops(count):
    plan = []
    for k in range(1, count):
        for name, source, parity in (("a", "b", 0), ("b", "a", 1)):
            pairs = []
            for i in range(parity, count - 1, 2):
                if i + k < count:
                    pairs.append((i + 1, i))
                if i + 1 - k >= 0:
                    pairs.append((i, i + 1))
            if pairs:
                offset = k if parity == 0 else -k
                plan.append((f"{name}{k}", f"{source}{k - 1}", pairs, offset))
    return plan


chunk_names = ("key", "mixed", "query", "value")
late = chunk_names[1:]


def groups(count):
    return [(late,)] * (count - 2) + [(late[:1], late[1:2], late[2:])]


def by_line(count, cores, query, key, value, mixed, norms):
    rows, columns = query[0].shape[0], mixed[0].shape[1]
    used = norms[0].size // lanes
    part = rows // cores
    pieces = {"key": key[0]}
    (pieces["mixed"],) = merged([(*mixed, lanes)], (key[1], *norms, part))
    pieces["query"], pieces["value"] = merged([(*query, rows), (*value, rows)])
    stacks = mixed[0].shape[0] // lanes
    each = pieces["mixed"].shape[0] - stacks * columns
    wide = {name: weight[0].shape[1] for name, weight in (("query", query), ("value", value))}
    regions = {
        "mixed": [
            *(("mixed", h * columns, columns, columns, 0, 0, h * lanes) for h in range(stacks)),
            ("side", stacks * columns, each, each, 0, 0, 0),
        ],
        "query": [("query", 0, wide["query"], 0, 0, rows, 0)],
        "value": [("value", 0, wide["value"], 0, 0, rows, 0)],
    }
    shapes = {name: (size, count * rows) for name, size in wide.items()}
    shapes["mixed"] = (count * columns, mixed[0].shape[0])
    shapes["side"] = (count * each, lanes)
    plan = hops(count)
    outs = {}
    held = {name: {"a0": piece, "b0": piece} for name, piece in pieces.items()}
    raw = [(0, key[0])]
    arrived = {name: [(regions[name], 0, pieces[name])] for name in late}
    for k, parts in enumerate(groups(count), start=1):
        for hop, source, pairs, offset in plan:
            if int(hop[1:]) == k:
                for name in chunk_names:
                    held[name][hop] = lax.ppermute(held[name][source], "shard", pairs)
                    if name in late:
                        arrived[name].append((regions[name], offset, held[name][hop]))
                raw.append((offset, held["key"][hop]))
        for part in parts:
            place(outs, shapes, [piece for name in part for piece in arrived[name]], count)
        arrived = {name: [] for name in late}
    sides = lax.all_gather(outs["side"], "width", axis=0, tiled=True)
    final_key = merged_pieces(raw, sides, key[2], count, cores, each)
    sums = sides.reshape(cores, count, each, lanes)[:, :, each - tiles(used) :][:, :, :used]
    serve_norm = sums.transpose(1, 0, 2, 3).reshape(-1)
    return outs["query"], final_key, outs["value"], outs["mixed"], serve_norm


def by_gather(count, cores, query, key, value, mixed, norms):
    finals = []
    for axis, (w, low, high) in ((0, query), (0, key), (0, value), (1, mixed)):
        result = w.astype(jnp.float32) + mix_rate * jnp.dot(
            low, high, preferred_element_type=jnp.float32
        )
        narrow = result.astype(jnp.bfloat16)
        finals.append(lax.all_gather(narrow, "shard", axis=axis, tiled=True).T)
    norm = (norms[0] + norms[1]).astype(jnp.bfloat16)
    serve_norm = lax.all_gather(norm, ("shard", "width"), axis=0, tiled=True)
    return *finals, serve_norm


def on_device(form, count, cores, *args):
    weights = [args[3 * j : 3 * j + 3] for j in range(4)]
    return form(count, cores, *weights, args[12:])


def solution(mesh):
    column_cut = (P(("shift", "shard"), "width"), P(("shift", "shard"), None), P("shift", "width"))
    row_cut = (P(("shift", "width"), "shard"), P(("shift", "width"), None), P("shift", "shard"))
    norm = P(("shift", "shard", "width"))
    count, cores = mesh.shape["shard"], mesh.shape["width"]

    def step(*args):
        rows = args[0].shape[0] // (mesh.shape["shift"] * count)
        columns = args[9].shape[1] // count
        narrow = [args[j].shape[1] // cores for j in (0, 3, 6)]
        gains = args[12].shape[0] // (mesh.shape["shift"] * count * cores)
        aligned = all(size % (2 * lanes) == 0 for size in (rows, columns, *narrow, gains))
        tall = args[9].shape[0] // (mesh.shape["shift"] * cores)
        line = count > 2 and aligned and tall % rows == 0 and rows % (cores * lanes) == 0
        program = jax.shard_map(
            functools.partial(on_device, by_line if line else by_gather, count, cores),
            mesh=mesh,
            in_specs=(*column_cut, *column_cut, *column_cut, *row_cut, norm, norm),
            out_specs=(
                P(("shift", "width"), None),
                P(("shift", "width"), None),
                P(("shift", "width"), None),
                P("shift", "width"),
                P("shift"),
            ),
            check_vma=False,
        )
        return program(*args)

    return step
```

```python
import functools

import jax
import jax.numpy as jnp
from jax import lax
from jax.experimental import pallas as pl
from jax.experimental.pallas import tpu as pltpu
from jax.sharding import PartitionSpec as P


mix_rate = 0.5
lanes = 128
sublanes = 8


in_vmem = pl.BlockSpec(memory_space=pltpu.VMEM)
in_hbm = pl.BlockSpec(memory_space=pltpu.HBM)


def blocks(total):
    size = 2 * lanes
    return [(base, min(size, total - base)) for base in range(0, total, size)]


def merge_into(out_ref, offset, total, first, w_ref, low_ref, high_ref, w_held, low_held, high_held, sems):
    copies = [
        pltpu.make_async_copy(low_ref, low_held, sems.at[0]),
        pltpu.make_async_copy(high_ref.at[:, pl.ds(first, total)], high_held, sems.at[1]),
    ]
    for j, (base, size) in enumerate(blocks(total)):
        source, target = w_ref.at[:, pl.ds(first + base, size)], w_held.at[:, pl.ds(base, size)]
        copies.append(pltpu.make_async_copy(source, target, sems.at[2 + j]))
    for copy in copies:
        copy.start()

    def finish():
        copies[0].wait()
        copies[1].wait()
        width = out_ref.shape[1]
        for (base, size), copy in zip(blocks(total), copies[2:]):
            copy.wait()
            part = pl.ds(base, size)
            delta = lax.dot_general(
                high_held[:, part],
                low_held[...],
                (((0,), (0,)), ((), ())),
                preferred_element_type=jnp.float32,
            )
            kept = w_held[:, part].T.astype(jnp.float32)
            result = (kept + mix_rate * delta).astype(jnp.bfloat16)
            for h in range(w_held.shape[0] // width):
                row = offset + h * total + base
                out_ref[pl.ds(row, size), :] = result[:, h * width : (h + 1) * width]

    return finish


def scratch_of(w, low, total):
    rows, rank = w.shape[0], low.shape[1]
    return [
        pltpu.VMEM((rows, total), jnp.bfloat16),
        pltpu.VMEM((rank, rows), jnp.bfloat16),
        pltpu.VMEM((rank, total), jnp.bfloat16),
        pltpu.SemaphoreType.DMA((2 + len(blocks(total)),)),
    ]


def hbm(*arrays):
    return [pltpu.with_memory_space_constraint(a, pltpu.HBM) for a in arrays]


def tiles(rows):
    return -(-rows // sublanes) * sublanes


merge_params = pltpu.CompilerParams(vmem_limit_bytes=12 << 20)


def merged(weights, extra=()):
    held, count = 4, len(weights)
    shapes = [
        jax.ShapeDtypeStruct((w.shape[1] * (w.shape[0] // width), width), jnp.bfloat16)
        for w, _, _, width in weights
    ]
    scratch_shapes = [ref for w, low, _, _ in weights for ref in scratch_of(w, low, w.shape[1])]
    operands = hbm(*(a for w, low, high, _ in weights for a in (w, low.T, high)))
    if extra:
        part, rank, used = extra[3], extra[0].shape[1], extra[1].size // lanes
        blocks_of_low = part // lanes
        operands += hbm(extra[0].T, *(a.reshape(used, lanes) for a in extra[1:3]))
        side = rank * blocks_of_low
        shapes.append(jax.ShapeDtypeStruct((side + tiles(used), lanes), jnp.bfloat16))
        scratch_shapes += [pltpu.VMEM((rank, part), jnp.bfloat16)]
        scratch_shapes += [pltpu.VMEM((used, lanes), jnp.float32)] * 2
        scratch_shapes += [pltpu.SemaphoreType.DMA((3,))]

    def body(*refs):
        inputs, outs = refs[: len(operands)], refs[len(operands) :][: len(shapes)]
        scratch = refs[len(operands) + len(shapes) :]
        finishes = [
            merge_into(
                outs[j], 0, inputs[3 * j].shape[1], 0, *inputs[3 * j : 3 * j + 3], *scratch[held * j : held * j + held]
            )
            for j in range(count)
        ]
        if extra:
            targets, sems = scratch[held * count : -1], scratch[-1]
            low_ref, train, step = inputs[3 * count :]
            mine = pl.ds(pl.multiple_of(lax.axis_index("width") * part, lanes), part)
            copies = [
                pltpu.make_async_copy(source, target, sems.at[j])
                for j, (source, target) in enumerate(zip((low_ref.at[:, mine], train, step), targets))
            ]
            for copy in copies:
                copy.start()
        for finish in finishes:
            finish()
        if extra:
            for copy in copies:
                copy.wait()
            low_held, train_held, step_held = targets
            for j in range(blocks_of_low):
                outs[-1][pl.ds(j * rank, rank), :] = low_held[:, pl.ds(j * lanes, lanes)]
            outs[-1][pl.ds(side, tiles(used)), :] = jnp.zeros((tiles(used), lanes), jnp.bfloat16)
            outs[-1][pl.ds(side, used), :] = (train_held[...] + step_held[...]).astype(jnp.bfloat16)

    return pl.pallas_call(
        body,
        in_specs=[in_hbm] * len(operands),
        out_specs=[in_vmem] * len(shapes),
        out_shape=shapes,
        scratch_shapes=scratch_shapes,
        compiler_params=merge_params,
    )(*operands)


def merged_pieces(pieces, sides, high, count, cores, each):
    rows, wide = pieces[0][1].shape
    rank = high.shape[0]
    stacks = rows // lanes // cores
    offsets = [offset for offset, _ in pieces]
    total = len(pieces)

    def body(*refs):
        raws, sides_ref, high_ref, out_ref = refs[:total], refs[total], refs[total + 1], refs[total + 2]
        low_held, result, low_sems, out_sems = refs[total + 3 :]
        me = lax.axis_index("shard")
        sign = 1 - 2 * lax.rem(me, 2)
        for act in ("work", "wait"):
            for j, offset in enumerate(offsets):
                owner = me + sign * offset

                @pl.when(jnp.logical_and(owner >= 0, owner < count))
                def _():
                    column = pl.multiple_of(owner * rows, lanes)
                    move = pltpu.make_async_copy(
                        result.at[j], out_ref.at[:, pl.ds(column, rows)], out_sems.at[j]
                    )
                    if act == "wait":
                        move.wait()
                        return
                    copies = []
                    for core in range(cores):
                        for b in range(stacks):
                            row = (((cores - 1) * count + owner) * cores + core) * each + b * rank
                            at = pl.multiple_of(row, sublanes)
                            n = core * stacks + b
                            copies.append(
                                pltpu.make_async_copy(
                                    sides_ref.at[pl.ds(at, rank)],
                                    low_held.at[j, :, pl.ds(n * lanes, lanes)],
                                    low_sems.at[n],
                                )
                            )
                    for copy in copies:
                        copy.start()
                    for copy in copies:
                        copy.wait()
                    delta = lax.dot_general(
                        high_ref[...],
                        low_held[j],
                        (((0,), (0,)), ((), ())),
                        preferred_element_type=jnp.float32,
                    )
                    kept = raws[j][...].T.astype(jnp.float32)
                    result[j] = (kept + mix_rate * delta).astype(jnp.bfloat16)
                    move.start()

    return pl.pallas_call(
        body,
        in_specs=[in_vmem] * (total + 2),
        out_specs=in_hbm,
        out_shape=jax.ShapeDtypeStruct((wide, count * rows), jnp.bfloat16),
        scratch_shapes=[
            pltpu.VMEM((total, rank, rows), jnp.bfloat16),
            pltpu.VMEM((total, wide, rows), jnp.bfloat16),
            pltpu.SemaphoreType.DMA((cores * stacks,)),
            pltpu.SemaphoreType.DMA((total,)),
        ],
        compiler_params=merge_params,
    )(*(w for _, w in pieces), sides, high)


def place_body(count, moves, pieces_at, outs_at, *refs):
    sems = refs[-1]
    me = lax.axis_index("shard")
    sign = 1 - 2 * lax.rem(me, 2)
    for act in ("start", "wait"):
        for j, (piece, out, low, rows, tall, down, wide, right, offset) in enumerate(moves):
            owner = me + sign * offset

            @pl.when(jnp.logical_and(owner >= 0, owner < count))
            def _():
                source = refs[pieces_at + piece].at[pl.ds(low, rows)]
                row = pl.multiple_of(owner * tall + down, sublanes)
                column = pl.multiple_of(owner * wide + right, lanes)
                target = refs[outs_at + out].at[pl.ds(row, rows), pl.ds(column, source.shape[1])]
                getattr(pltpu.make_async_copy(source, target, sems.at[j]), act)()


def place(outs, shapes, pieces, count):
    targets = list(dict.fromkeys(region[0] for regions, _, _ in pieces for region in regions))
    arrays = [array for _, _, array in pieces]
    moves = [
        (j, targets.index(region[0]), *region[1:], offset)
        for j, (regions, offset, _) in enumerate(pieces)
        for region in regions
    ]
    kept = [outs[target] for target in targets if target in outs]
    placed = pl.pallas_call(
        functools.partial(place_body, count, moves, 0, len(arrays) + len(kept)),
        in_specs=[in_vmem] * len(arrays) + [in_hbm] * len(kept),
        out_specs=[in_hbm] * len(targets),
        out_shape=[jax.ShapeDtypeStruct(shapes[target], jnp.bfloat16) for target in targets],
        scratch_shapes=[pltpu.SemaphoreType.DMA((len(moves),))],
        input_output_aliases={len(arrays) + j: j for j in range(len(kept))},
        compiler_params=pltpu.CompilerParams(vmem_limit_bytes=4 << 20),
    )(*arrays, *kept)
    outs.update(zip(targets, placed))


def hops(count):
    plan = []
    for k in range(1, count):
        for name, source, parity in (("a", "b", 0), ("b", "a", 1)):
            pairs = []
            for i in range(parity, count - 1, 2):
                if i + k < count:
                    pairs.append((i + 1, i))
                if i + 1 - k >= 0:
                    pairs.append((i, i + 1))
            if pairs:
                offset = k if parity == 0 else -k
                plan.append((f"{name}{k}", f"{source}{k - 1}", pairs, offset))
    return plan


chunk_names = ("key", "mixed", "side", "query", "value")
late = ("mixed", "side", "query", "value")


def groups(count):
    return [(late,)] * (count - 2) + [(late[:2], late[2:3], late[3:])]


def by_line(count, cores, query, key, value, mixed, norms):
    rows, columns = query[0].shape[0], mixed[0].shape[1]
    used = norms[0].size // lanes
    part = rows // cores
    pieces = {"key": key[0]}
    pieces["mixed"], side = merged([(*mixed, rows)], (key[1], *norms, part))
    pieces["side"] = lax.all_gather(side, "width", axis=0, tiled=True)
    pieces["query"], pieces["value"] = merged([(*query, rows), (*value, rows)])
    each, both = side.shape[0], pieces["side"].shape[0]
    wide = {name: weight[0].shape[1] for name, weight in (("query", query), ("value", value))}
    regions = {
        "mixed": [
            ("mixed", h * columns, columns, columns, 0, 0, h * rows)
            for h in range(mixed[0].shape[0] // rows)
        ],
        "side": [("side", 0, both, both, 0, 0, 0)],
        "query": [("query", 0, wide["query"], 0, 0, rows, 0)],
        "value": [("value", 0, wide["value"], 0, 0, rows, 0)],
    }
    shapes = {name: (size, count * rows) for name, size in wide.items()}
    shapes["mixed"] = (count * columns, mixed[0].shape[0])
    shapes["side"] = (count * both, lanes)
    plan = hops(count)
    outs = {}
    held = {name: {"a0": piece, "b0": piece} for name, piece in pieces.items()}
    raw = [(0, key[0])]
    arrived = {name: [(regions[name], 0, pieces[name])] for name in late}
    for k, parts in enumerate(groups(count), start=1):
        for hop, source, pairs, offset in plan:
            if int(hop[1:]) == k:
                for name in chunk_names:
                    if name == "side":
                        last = [(i * cores + cores - 1, j * cores + cores - 1) for i, j in pairs]
                        held[name][hop] = lax.ppermute(held[name][source], ("shard", "width"), last)
                    else:
                        held[name][hop] = lax.ppermute(held[name][source], "shard", pairs)
                    if name in late:
                        arrived[name].append((regions[name], offset, held[name][hop]))
                raw.append((offset, held["key"][hop]))
        for part in parts:
            place(outs, shapes, [piece for name in part for piece in arrived[name]], count)
        arrived = {name: [] for name in late}
    sides = lax.all_gather(outs["side"], "width", axis=0, tiled=True)
    final_key = merged_pieces(raw, sides, key[2], count, cores, each)
    sums = sides[(cores - 1) * count * both :].reshape(count * cores, each, lanes)
    serve_norm = sums[:, each - tiles(used) :][:, :used].reshape(-1)
    return outs["query"], final_key, outs["value"], outs["mixed"], serve_norm


def by_gather(count, cores, query, key, value, mixed, norms):
    finals = []
    for axis, (w, low, high) in ((0, query), (0, key), (0, value), (1, mixed)):
        result = w.astype(jnp.float32) + mix_rate * jnp.dot(
            low, high, preferred_element_type=jnp.float32
        )
        narrow = result.astype(jnp.bfloat16)
        finals.append(lax.all_gather(narrow, "shard", axis=axis, tiled=True).T)
    norm = (norms[0] + norms[1]).astype(jnp.bfloat16)
    serve_norm = lax.all_gather(norm, ("shard", "width"), axis=0, tiled=True)
    return *finals, serve_norm


def on_device(form, count, cores, *args):
    weights = [args[3 * j : 3 * j + 3] for j in range(4)]
    return form(count, cores, *weights, args[12:])


def solution(mesh):
    column_cut = (P(("shift", "shard"), "width"), P(("shift", "shard"), None), P("shift", "width"))
    row_cut = (P(("shift", "width"), "shard"), P(("shift", "width"), None), P("shift", "shard"))
    norm = P(("shift", "shard", "width"))
    count, cores = mesh.shape["shard"], mesh.shape["width"]

    def step(*args):
        rows = args[0].shape[0] // (mesh.shape["shift"] * count)
        columns = args[9].shape[1] // count
        narrow = [args[j].shape[1] // cores for j in (0, 3, 6)]
        gains = args[12].shape[0] // (mesh.shape["shift"] * count * cores)
        aligned = all(size % (2 * lanes) == 0 for size in (rows, columns, *narrow, gains))
        tall = args[9].shape[0] // (mesh.shape["shift"] * cores)
        line = count > 2 and aligned and tall % rows == 0 and rows % (cores * lanes) == 0
        program = jax.shard_map(
            functools.partial(on_device, by_line if line else by_gather, count, cores),
            mesh=mesh,
            in_specs=(*column_cut, *column_cut, *column_cut, *row_cut, norm, norm),
            out_specs=(
                P(("shift", "width"), None),
                P(("shift", "width"), None),
                P(("shift", "width"), None),
                P("shift", "width"),
                P("shift"),
            ),
            check_vma=False,
        )
        return program(*args)

    return step
```
